128 devices in a mesh: seq: 32 (over y_lo, z, x), head: 4 (over y_hi, core).
Axes of the slice: x: 4, y: 4 (y_hi: 2, y_lo: 2; y = y_hi * 2 + y_lo), z: 4, core: 2. Of those that a mesh axis runs over, the one named last changes fastest.
Arguments:
- queries: bfloat16 [4096, 3072], P('seq', 'head'), may hold values from -8 to 8
- latents: bfloat16 [4096, 576], P('seq'), may hold values from -8 to 8
- key_up: bfloat16 [512, 2048], P(None, 'head'), may hold values from -0.25 to 0.25
- value_up: bfloat16 [512, 2048], P(None, 'head'), may hold values from -0.25 to 0.25
- out_grad: bfloat16 [4096, 2048], P('seq', 'head'), may hold values from -48 to 48
- positions: int32 [4096], P('seq'), may hold values from 0 to 4095, as said below
Outputs:
- query_grad: bfloat16 [4096, 3072], P('seq', 'head')
- latent_grad: float32 [4096, 576], P('seq')
- key_up_grad: float32 [512, 2048], P(None, 'head')
- value_up_grad: float32 [512, 2048], P(None, 'head')
The draws below stay inside these ranges and needn't reach their ends.
Inputs may be any that keep to these rules, and one draw needn't show every extreme that they name: Every position from 0 to 4095 occurs once; positions come in stripes of 128 consecutive positions in ascending order, each stripe whole within the rows of one device.
All inputs are finite; a program needn't handle non-finite values.
Results may differ from the reference program's by a relative error of at most 0.0084.
Values may be sent and summed in bfloat16 or wider, within the bound.
No kernel may reach another device: no remote copies, remote signals or barrier semaphores. Data moves between devices by JAX's collectives and lax.ppermute only.
A program may use at most 64 MiB of HBM per device.

```python
import math
import jax
import jax.numpy as jnp
from jax import lax

D_LAT = 512
D_ROPE = 64
D_NOPE = 128
D_V = 128
STRIPE = 128
HEADS = 16
SEQ = 4096


def stripe_positions(key):
    order = jax.random.permutation(jax.random.fold_in(key, 11), SEQ // STRIPE).astype(jnp.int32)
    within = jnp.arange(STRIPE, dtype=jnp.int32)
    return (order[:, None] * STRIPE + within[None, :]).reshape(SEQ)


def draw_positions(key, part):
    return stripe_positions(key)


def draw_queries(key, part):
    width = HEADS * (D_NOPE + D_ROPE)
    own = jax.random.fold_in(key, 21)
    base = jax.random.normal(own, (SEQ, width), jnp.float32)
    return jnp.clip(base, -8.0, 8.0).astype(jnp.bfloat16)


def draw_latents(key, part):
    width = D_LAT + D_ROPE
    own = jax.random.fold_in(key, 31)
    base = jax.random.normal(own, (SEQ, width), jnp.float32)
    return jnp.clip(base, -8.0, 8.0).astype(jnp.bfloat16)


def block_levels(stream_key, extent, pieces, least, top_value):
    factor_of = 1.0
    for position, shards_of in pieces:
        steps = jax.random.uniform(jax.random.fold_in(jax.random.fold_in(stream_key, 6), position), (shards_of,), jnp.float32, least / len(pieces), top_value / len(pieces))
        factor_of = factor_of * jnp.repeat(jnp.exp(steps), extent[position] // shards_of).reshape((-1,) + (1,) * (len(extent) - 1 - position))
    return factor_of


def normal_values(own_key, dims, deviation, limit, pieces=(), held_as=jnp.bfloat16):
    factor_of = block_levels(own_key, dims, pieces, -0.22, 0.18) if pieces else 1.0
    entries = jax.random.normal(own_key, dims, jnp.float32) * deviation * factor_of
    return jnp.minimum(jnp.maximum(entries, -limit), limit).astype(held_as)


def setup_inputs(seed: int = 0) -> dict:
    key_of = jax.random.split(jax.random.key(seed), 7)
    return {
        "queries": draw_queries(jax.random.fold_in(key_of[6], 71), 0),
        "latents": draw_latents(jax.random.fold_in(key_of[6], 71), 0),
        "key_up": normal_values(key_of[2], (D_LAT, HEADS * D_NOPE), D_LAT ** -0.5, 0.25, ((1, 4),)),
        "value_up": normal_values(key_of[3], (D_LAT, HEADS * D_V), D_LAT ** -0.5, 0.25, ((1, 4),)),
        "out_grad": normal_values(key_of[4], (SEQ, HEADS * D_V), 8.0, 48.0, ((0, 32), (1, 4))),
        "positions": draw_positions(jax.random.fold_in(key_of[6], 71), 0),
    }


NEG = -1e+30

def reference(queries, latents, key_up, value_up, out_grad, positions):
    seq = latents.shape[0]
    heads = key_up.shape[1] // D_NOPE
    qk = D_NOPE + D_ROPE
    scale = 1.0 / math.sqrt(qk)
    compressed = latents[:, :D_LAT]
    rope_keys = latents[:, D_LAT:].astype(jnp.float32)
    key_nope = jnp.dot(compressed, key_up, preferred_element_type=jnp.float32).astype(jnp.bfloat16)
    values = jnp.dot(compressed, value_up, preferred_element_type=jnp.float32).astype(jnp.bfloat16)
    key_heads = lax.optimization_barrier(key_nope).astype(jnp.float32).reshape(seq, heads, D_NOPE)
    value_heads = lax.optimization_barrier(values).astype(jnp.float32).reshape(seq, heads, D_V)
    block = math.gcd(seq, 512)
    nblocks = seq // block
    q_blocks = queries.reshape(nblocks, block, heads, qk)
    g_blocks = out_grad.reshape(nblocks, block, heads, D_V)
    p_blocks = positions.reshape(nblocks, block)

    def one_block(carry, inputs):
        key_acc, rope_acc, value_acc = carry
        q_block, g_block, pos_block = inputs
        q_nope = q_block[:, :, :D_NOPE].astype(jnp.float32)
        q_rope = q_block[:, :, D_NOPE:].astype(jnp.float32)
        grads = g_block.astype(jnp.float32)
        scores = jnp.einsum('bhd,khd->hbk', q_nope, key_heads)
        scores = (scores + jnp.einsum('bhd,kd->hbk', q_rope, rope_keys)) * scale
        visible = (positions[None, :] <= pos_block[:, None])[None]
        masked = jnp.where(visible, scores, NEG)
        top = lax.optimization_barrier(jnp.max(masked, axis=2, keepdims=True))
        total = lax.optimization_barrier(jnp.sum(jnp.exp(jnp.where(visible, scores - top, NEG)), axis=2, keepdims=True))
        lse = top + jnp.log(total)
        probs = jnp.exp(jnp.where(visible, scores - lse, NEG))
        dprobs = jnp.einsum('bhd,khd->hbk', grads, value_heads)
        delta = lax.optimization_barrier(jnp.sum(probs * dprobs, axis=2, keepdims=True))
        dscore16 = (probs * (dprobs - delta) * scale).astype(jnp.bfloat16)
        dscore = lax.optimization_barrier(dscore16).astype(jnp.float32)
        probs16 = lax.optimization_barrier(probs.astype(jnp.bfloat16)).astype(jnp.float32)
        grad_nope = jnp.einsum('hbk,khd->bhd', dscore, key_heads)
        grad_rope = jnp.einsum('hbk,kd->bhd', dscore, rope_keys)
        q_grad = jnp.concatenate([grad_nope, grad_rope], axis=2).reshape(block, heads * qk)
        key_acc = key_acc + jnp.einsum('hbk,bhd->khd', dscore, q_nope)
        rope_acc = rope_acc + jnp.einsum('hbk,bhd->kd', dscore, q_rope)
        value_acc = value_acc + jnp.einsum('hbk,bhd->khd', probs16, grads)
        return ((key_acc, rope_acc, value_acc), q_grad.astype(jnp.bfloat16))
    start = (jnp.zeros((seq, heads, D_NOPE), jnp.float32), jnp.zeros((seq, D_ROPE), jnp.float32), jnp.zeros((seq, heads, D_V), jnp.float32))
    sums, q_grads = lax.scan(one_block, start, (q_blocks, g_blocks, p_blocks))
    key_acc, rope_acc, value_acc = sums
    key_grad = key_acc.reshape(seq, heads * D_NOPE)
    value_grad = value_acc.reshape(seq, heads * D_V)
    high = lax.Precision.HIGHEST
    key_up32 = key_up.astype(jnp.float32)
    value_up32 = value_up.astype(jnp.float32)
    folded = jnp.dot(key_grad, key_up32.T, precision=high)
    folded = folded + jnp.dot(value_grad, value_up32.T, precision=high)
    latent_grad = jnp.concatenate([folded, rope_acc], axis=1)
    compressed32 = compressed.astype(jnp.float32)
    key_up_grad = jnp.dot(compressed32.T, key_grad, precision=high)
    value_up_grad = jnp.dot(compressed32.T, value_grad, precision=high)
    query_grad = q_grads.reshape(seq, heads * qk)
    return (query_grad, latent_grad, key_up_grad, value_up_grad)
```

```python
import functools
import math

import jax
import jax.numpy as jnp
from jax import lax
from jax.experimental import pallas as pl
from jax.experimental.pallas import tpu as pltpu
from jax.sharding import PartitionSpec as P

BF = jnp.bfloat16
F32 = jnp.float32
D_LAT = 512
D_ROPE = 64
D_NOPE = 128
D_V = 128
ROWS = 128
SCALE = 1.0 / math.sqrt(D_NOPE + D_ROPE)
SCALE2 = SCALE * math.log2(math.e)
NEG = -1e30
QP = 336
LP = 592
NQ = 2048
NK = 1024
TQ = 256


def place(y, z, x):
    return (y % 2) * 16 + (z % 4) * 4 + x % 4


def along(value, dy=0, dz=0, dx=0):
    pairs = [
        (place(y, z, x), place(y + dy, z + dz, x + dx))
        for y in range(2)
        for z in range(4)
        for x in range(4)
    ]
    return lax.ppermute(value, "seq", pairs)


def rounded(value):
    return lax.reduce_precision(value, 8, 7)


X_GROUPS = [[4 * k + i for i in range(4)] for k in range(8)]


def call(kernel, outs, *args, scratch=(), smem=0, flops=0, name=None):
    vm = pl.BlockSpec(memory_space=pltpu.VMEM)
    sm = pl.BlockSpec(memory_space=pltpu.SMEM)
    return pl.pallas_call(
        kernel,
        out_shape=[jax.ShapeDtypeStruct(s, d) for s, d in outs],
        in_specs=[sm] * smem + [vm] * (len(args) - smem),
        out_specs=[vm] * len(outs),
        scratch_shapes=list(scratch),
        cost_estimate=pl.CostEstimate(flops=max(flops, 1), bytes_accessed=1 << 20, transcendentals=0),
        compiler_params=pltpu.CompilerParams(vmem_limit_bytes=56 << 20),
        name=name,
    )(*args)


def dense_rope(block):
    return jnp.concatenate([block[0:64], block[64:128]], axis=1)


def wide_rope(block):
    return jnp.concatenate([block[:, 0:64], block[:, 64:128]], axis=0)


def pack_latents(idx, lat, out):
    for j in range(4):
        out[128 * j : 128 * (j + 1)] = lat[:, 128 * j : 128 * (j + 1)]
    out[512:576] = dense_rope(lat[:, 512:576])
    out[576:592] = jnp.full((16, 128), idx[0].astype(F32), F32).astype(BF)


def pack_queries(idx, q, g, out):
    tag = jnp.full((16, 128), idx[0].astype(F32), F32).astype(BF)
    for h in range(4):
        out[h, 0:128] = q[:, 192 * h : 192 * h + 128]
        out[h, 128:256] = g[:, 128 * h : 128 * h + 128]
        out[h, 256:320] = dense_rope(q[:, 192 * h + 128 : 192 * h + 192])
        out[h, 320:336] = tag


def visible(qtag, ktag, late):
    return late <= (qtag - ktag) * 128.0


def masked_scores(raw, qtags, ktags, late):
    rows = []
    for kb in range(NK // 128):
        cols = []
        for qb in range(TQ // 128):
            part = raw[128 * kb : 128 * kb + 128, 128 * qb : 128 * qb + 128]
            cols.append(jnp.where(visible(qtags[qb], ktags[kb], late), part * SCALE2, NEG))
        rows.append(jnp.concatenate(cols, axis=1))
    return jnp.concatenate(rows, axis=0)


def lateness():
    shape = (128, 128)
    return (lax.broadcasted_iota(jnp.int32, shape, 0) - lax.broadcasted_iota(jnp.int32, shape, 1)).astype(F32)


NT = (((1,), (1,)), ((), ()))
NN = (((1,), (0,)), ((), ()))
TN = (((0,), (0,)), ((), ()))


def mm(a, b, dims):
    return lax.dot_general(a, b, dims, preferred_element_type=F32)


def forward(q0, qa, qb, qc, qd, l0, l1, la, lb, lc, ld, ku, vu, qp, do, qtag, comp, kp, kpt, v, ktag, stats):
    blocks = [q0[i] for i in range(4)] + [qb[i] for i in range(4)]
    blocks += [qc[0], qc[1], qd[0], qd[1]] + [qa[i] for i in range(4)]
    zeros = jnp.zeros((128, 64), BF)
    for n, block in enumerate(blocks):
        at = 128 * n
        qp[at : at + 128, 0:128] = block[0:128]
        qp[at : at + 128, 128:256] = jnp.concatenate([wide_rope(block[256:320]), zeros], axis=1)
        do[at : at + 128] = block[128:256]
        qtag[0:8, at : at + 128] = block[320:336].astype(F32)[0:8]
    keys = [l0[...], l1[...], lb[0], lb[1], lc[0], ld[0], la[0], la[1]]
    for n, block in enumerate(keys):
        at = 128 * n
        for j in range(4):
            comp[at : at + 128, 128 * j : 128 * (j + 1)] = block[128 * j : 128 * (j + 1)]
        kp[at : at + 128, 128:256] = jnp.concatenate([wide_rope(block[512:576]), zeros], axis=1)
        ktag[8 * n : 8 * n + 8] = block[576:592].astype(F32)[0:8]
    kp[:, 0:128] = mm(comp[...], ku[...], NN).astype(BF)
    v[...] = mm(comp[...], vu[...], NN).astype(BF)
    kpt[...] = kp[...].T
    late = lateness()
    ktags = [ktag[8 * n : 8 * n + 1] for n in range(8)]

    def turn(i, carry):
        at = pl.multiple_of(i * TQ, TQ)
        raw = mm(kp[...], qp[pl.ds(at, TQ)], NT)
        qt = qtag[0:1, pl.ds(at, TQ)]
        s = masked_scores(raw, [qt[:, 0:128], qt[:, 128:256]], ktags, late)
        top = jnp.max(s, axis=0, keepdims=True)
        p = jnp.exp2(s - top)
        dp = mm(v[...], do[pl.ds(at, TQ)], NT)
        stats[0:1, pl.ds(at, TQ)] = top
        stats[1:2, pl.ds(at, TQ)] = jnp.sum(p, axis=0, keepdims=True)
        stats[2:3, pl.ds(at, TQ)] = jnp.sum(p * dp, axis=0, keepdims=True)
        return carry

    stats[...] = jnp.zeros_like(stats)
    lax.fori_loop(0, NQ // TQ, turn, 0)


def backward(z, qp, do, qtag, comp, kp, kpt, v, ktag, s0, s1, s2, s3, zpay, xpay, dk, dv, low, up):
    late = lateness()
    ktags = [ktag[8 * n : 8 * n + 1] for n in range(8)]
    stats = [s0, s1, s2, s3]
    for r in range(4):
        rows = []
        for d in range(4):
            at = 512 * ((r - d) % 4)
            rows.append([stats[d][n : n + 1, at : at + 512] for n in range(3)])
        top = functools.reduce(jnp.maximum, [t[0] for t in rows])
        total = sum(t[1] * jnp.exp2(t[0] - top) for t in rows)
        weighted = sum(t[2] * jnp.exp2(t[0] - top) for t in rows)
        low[0:1, 512 * r : 512 * r + 512] = top + jnp.log2(total)
        low[1:2, 512 * r : 512 * r + 512] = weighted / total
    dk[...] = jnp.zeros_like(dk)
    dv[...] = jnp.zeros_like(dv)
    for i in range(NQ // TQ):
        at = i * TQ
        q = qp[at : at + TQ]
        g = do[at : at + TQ]
        raw = mm(kp[...], q, NT)
        qt = qtag[0:1, at : at + TQ]
        s = masked_scores(raw, [qt[:, 0:128], qt[:, 128:256]], ktags, late)
        p = jnp.exp2(s - low[0:1, at : at + TQ])
        dp = mm(v[...], g, NT)
        ds = (p * (dp - low[1:2, at : at + TQ])).astype(BF)
        dk[...] += mm(ds, q, NN)
        dv[...] += mm(p.astype(BF), g, NN)
        dq = (mm(kpt[...], ds, NN).T * SCALE).astype(BF)
        for b in range(TQ // 128):
            n = i * (TQ // 128) + b
            r, m = n // 4, n % 4
            zpay[r, 128 * m : 128 * m + 128] = dq[128 * b : 128 * b + 128, 0:128]
            zpay[r, 512 + 64 * m : 576 + 64 * m] = dense_rope(dq[128 * b : 128 * b + 128, 128:192])
    dk16 = (dk[...] * SCALE).astype(BF)
    dv16 = dv[...].astype(BF)
    for n in range(8):
        r, m = n // 2, n % 2
        xpay[r, 128 * m : 128 * m + 128] = dk16[128 * n : 128 * n + 128, 0:128]
        xpay[r, 256 + 128 * m : 384 + 128 * m] = dv16[128 * n : 128 * n + 128]
        xpay[r, 512 + 64 * m : 576 + 64 * m] = dense_rope(dk16[128 * n : 128 * n + 128, 128:192])
    both = jnp.concatenate([dk16[:, 0:128], dv16], axis=1)
    up[...] = mm(comp[...], both, TN).astype(BF)
    for r in range(4):
        at = pl.multiple_of(lax.rem(z[0] + r, 4) * 128, 128)
        part = up[pl.ds(at, 128)]
        zpay[r, 768:896] = part[:, 0:128]
        zpay[r, 896:1024] = part[:, 128:256]


def fold(x, p0, p1, p2, p3, ku, vu, own, other):
    acc = jnp.zeros((256, 512), F32)
    rope = jnp.zeros((128, 128), F32)
    for r, p in enumerate((p0, p1, p2, p3)):
        h = pl.multiple_of(lax.rem(x[0] + 4 - r, 4) * 128, 128)
        acc += mm(p[0:256], ku[:, pl.ds(h, 128)], NT)
        acc += mm(p[256:512], vu[:, pl.ds(h, 128)], NT)
        rope += p[512:640].astype(F32)
    for j in range(4):
        own[128 * j : 128 * j + 128] = acc[0:128, 128 * j : 128 * j + 128]
        other[128 * j : 128 * j + 128] = acc[128:256, 128 * j : 128 * j + 128].astype(BF)
    own[512:576] = rope[0:64]
    other[512:576] = rope[64:128].astype(BF)


def unpack_latent_grad(a, b, out):
    total = a[...].astype(F32) + b[...].astype(F32)
    for j in range(4):
        out[:, 128 * j : 128 * j + 128] = total[128 * j : 128 * j + 128]
    out[:, 512:576] = wide_rope(total[512:576])


def unpack_query_grad(a, out):
    for h in range(4):
        out[:, 192 * h : 192 * h + 128] = a[h, 0:128]
        out[:, 192 * h + 128 : 192 * h + 192] = wide_rope(a[h, 128:192])


def unpack_up(a, key, value):
    for y in range(2):
        for z in range(4):
            for x in range(4):
                part = a[place(y, z, x)].astype(F32)
                at = 128 * z + 64 * y
                key[at : at + 64, 128 * x : 128 * x + 128] = part[:, 0:128]
                value[at : at + 64, 128 * x : 128 * x + 128] = part[:, 128:256]


def shards(queries, latents, key_up, value_up, out_grad, positions):
    here = lax.axis_index("seq")
    y, z, x = here // 16, (here // 4) % 4, here % 4
    stripe = (positions[0:1] // ROWS).astype(jnp.int32)
    (lat,) = call(pack_latents, [((LP, 128), BF)], stripe, latents, smem=1, name="pack_latents")
    (qpk,) = call(pack_queries, [((4, QP, 128), BF)], stripe, queries, out_grad, smem=1, name="pack_queries")
    ku = lax.dynamic_slice(key_up, (0, x * 128), (D_LAT, 128))
    vu = lax.dynamic_slice(value_up, (0, x * 128), (D_LAT, 128))

    lat_y = along(lat, dy=1)
    q0 = lax.all_to_all(qpk, "seq", 0, 0, tiled=True, axis_index_groups=X_GROUPS)
    qa = along(q0, dz=1)
    qb = along(q0, dz=-1)
    pair = jnp.stack([lat, lat_y])
    la = along(pair, dx=1)
    lb = along(pair, dx=-1)
    qc = along(qa[:2], dz=1)
    qd = along(qb[2:], dz=-1)
    lc = along(la[:1], dx=1)
    ld = along(lb[1:], dx=-1)

    flops = 2 * NQ * NK * 512
    outs = [
        ((NQ, 256), BF), ((NQ, 128), BF), ((8, NQ), F32), ((NK, 512), BF), ((NK, 256), BF),
        ((256, NK), BF), ((NK, 128), BF), ((64, 128), F32), ((8, NQ), F32),
    ]
    made = call(forward, outs, q0, qa, qb, qc, qd, lat, lat_y, la, lb, lc, ld, ku, vu, flops=flops, name="forward")
    stats = made[8]
    s3 = along(stats, dz=1)
    s1 = along(stats, dz=-1)
    s2 = along(stats, dz=2)

    zpay, xpay = call(
        backward,
        [((4, 1024, 128), BF), ((4, 640, 128), BF)],
        z[None].astype(jnp.int32), *made[:8], stats, s1, s2, s3,
        scratch=[
            pltpu.VMEM((NK, 256), F32), pltpu.VMEM((NK, 128), F32),
            pltpu.VMEM((8, NQ), F32), pltpu.VMEM((512, 256), BF),
        ],
        smem=1, flops=3 * flops, name="backward",
    )
    zr = [along(zpay[r], dz=r) for r in (1, 2, 3)]
    xr = [along(xpay[r], dx=r) for r in (1, 2, 3)]

    zsum = zpay[0].astype(F32) + zr[0].astype(F32) + zr[1].astype(F32) + zr[2].astype(F32)
    up = jnp.concatenate([zsum[768:896], zsum[896:1024]], axis=1)
    kept = lax.dynamic_slice(up, (y * 64, 0), (64, 256))
    given = lax.dynamic_slice(up, ((1 - y) * 64, 0), (64, 256)).astype(BF)
    up_own = (kept + along(given, dy=1).astype(F32)).astype(BF)

    qsum = zsum[:768].astype(BF)
    qback = jnp.concatenate([qsum[:512].reshape(4, 128, 128), qsum[512:].reshape(4, 64, 128)], axis=1)
    qhome = lax.all_to_all(qback, "seq", 0, 0, tiled=True, axis_index_groups=X_GROUPS)
    (query_grad,) = call(unpack_query_grad, [((ROWS, 768), BF)], qhome, name="unpack_query_grad")

    own, other = call(
        fold, [((576, 128), F32), ((576, 128), BF)],
        x[None].astype(jnp.int32), xpay[0], *xr, key_up, value_up, smem=1, flops=2 * 256 * 512 * 1024, name="fold",
    )
    part = rounded(own + along(other, dy=1).astype(F32))
    near = lax.ppermute(part.astype(BF), "head", [(0, 1), (1, 0), (2, 3), (3, 2)])
    part = rounded(part + near.astype(F32)).astype(BF)
    far = lax.ppermute(part, "head", [(0, 2), (1, 3), (2, 0), (3, 1)])
    (latent_grad,) = call(unpack_latent_grad, [((ROWS, 576), F32)], part, far, name="unpack_latent_grad")

    every = lax.all_to_all(jnp.broadcast_to(up_own[None], (32, 64, 256)), "seq", 0, 0, tiled=True)
    key_up_grad, value_up_grad = call(
        unpack_up, [((512, 512), F32), ((512, 512), F32)], every, name="unpack_up"
    )
    return (query_grad, latent_grad, key_up_grad, value_up_grad)


def solution(mesh):
    in_specs = (
        P("seq", "head"),
        P("seq", None),
        P(None, "head"),
        P(None, "head"),
        P("seq", "head"),
        P("seq"),
    )
    out_specs = (P("seq", "head"), P("seq", None), P(None, "head"), P(None, "head"))
    return jax.shard_map(shards, mesh=mesh, in_specs=in_specs, out_specs=out_specs, check_vma=False)
```

```python
import functools
import math

import jax
import jax.numpy as jnp
from jax import lax
from jax.experimental import pallas as pl
from jax.experimental.pallas import tpu as pltpu
from jax.sharding import PartitionSpec as P

BF = jnp.bfloat16
F32 = jnp.float32
D_LAT = 512
D_ROPE = 64
D_NOPE = 128
D_V = 128
ROWS = 128
SCALE = 1.0 / math.sqrt(D_NOPE + D_ROPE)
SCALE2 = SCALE * math.log2(math.e)
NEG = -1e30
QP = 336
LP = 592
NQ = 2048
NK = 1024
TQ = 256


def place(y, z, x):
    return (y % 2) * 16 + (z % 4) * 4 + x % 4


def along(value, dy=0, dz=0, dx=0):
    pairs = [
        (place(y, z, x), place(y + dy, z + dz, x + dx))
        for y in range(2)
        for z in range(4)
        for x in range(4)
    ]
    return lax.ppermute(value, "seq", pairs)


def rounded(value):
    return lax.reduce_precision(value, 8, 7)


X_GROUPS = [[4 * k + i for i in range(4)] for k in range(8)]


def call(kernel, outs, *args, scratch=(), smem=0, flops=0, grant=6, name=None):
    vm = pl.BlockSpec(memory_space=pltpu.VMEM)
    sm = pl.BlockSpec(memory_space=pltpu.SMEM)
    return pl.pallas_call(
        kernel,
        out_shape=[jax.ShapeDtypeStruct(s, d) for s, d in outs],
        in_specs=[sm] * smem + [vm] * (len(args) - smem),
        out_specs=[vm] * len(outs),
        scratch_shapes=list(scratch),
        cost_estimate=pl.CostEstimate(flops=max(flops, 1), bytes_accessed=1 << 20, transcendentals=0),
        compiler_params=pltpu.CompilerParams(vmem_limit_bytes=grant << 20),
        name=name,
    )(*args)


def dense_rope(block):
    return jnp.concatenate([block[0:64], block[64:128]], axis=1)


def wide_rope(block):
    return jnp.concatenate([block[:, 0:64], block[:, 64:128]], axis=0)


def pack_queries(idx, q, g, out):
    tag = jnp.full((16, 128), idx[0].astype(F32), F32).astype(BF)
    for h in range(4):
        out[h, 0:128] = q[:, 192 * h : 192 * h + 128]
        out[h, 128:256] = g[:, 128 * h : 128 * h + 128]
        out[h, 256:320] = dense_rope(q[:, 192 * h + 128 : 192 * h + 192])
        out[h, 320:336] = tag


def masked_scores(raw, qtags, ktags, late):
    rows = []
    for kb in range(NK // 128):
        cols = []
        for qb in range(TQ // 128):
            part = raw[128 * kb : 128 * kb + 128, 128 * qb : 128 * qb + 128]
            seen = late <= (qtags[qb] - ktags[kb]) * 128.0
            cols.append(jnp.where(seen, part * SCALE2, NEG))
        rows.append(jnp.concatenate(cols, axis=1))
    return jnp.concatenate(rows, axis=0)


def lateness():
    shape = (128, 128)
    return (lax.broadcasted_iota(jnp.int32, shape, 0) - lax.broadcasted_iota(jnp.int32, shape, 1)).astype(F32)


NT = (((1,), (1,)), ((), ()))
NN = (((1,), (0,)), ((), ()))


def mm(a, b, dims):
    return lax.dot_general(a, b, dims, preferred_element_type=F32)


def take_queries(blocks, qp, do, qtag):
    zeros = jnp.zeros((128, 64), BF)
    for n, block in enumerate(blocks):
        at = 128 * n
        qp[at : at + 128, 0:128] = block[0:128]
        qp[at : at + 128, 128:256] = jnp.concatenate([wide_rope(block[256:320]), zeros], axis=1)
        do[at : at + 128] = block[128:256]
        qtag[0:8, at : at + 128] = block[320:336].astype(F32)[0:8]


def statistics(rows, qp, do, qtag, kp, v, ktag, stats, first):
    late = lateness()
    ktags = [ktag[8 * n : 8 * n + 1] for n in range(8)]

    def turn(i, carry):
        at = pl.multiple_of(i * TQ, TQ)
        to = pl.multiple_of(first + i * TQ, TQ)
        raw = mm(kp[...], qp[pl.ds(at, TQ)], NT)
        qt = qtag[0:1, pl.ds(at, TQ)]
        s = masked_scores(raw, [qt[:, 0:128], qt[:, 128:256]], ktags, late)
        top = jnp.max(s, axis=0, keepdims=True)
        p = jnp.exp2(s - top)
        dp = mm(v[...], do[pl.ds(at, TQ)], NT)
        stats[0:1, pl.ds(to, TQ)] = top
        stats[1:2, pl.ds(to, TQ)] = jnp.sum(p, axis=0, keepdims=True)
        stats[2:3, pl.ds(to, TQ)] = jnp.sum(p * dp, axis=0, keepdims=True)
        return carry

    lax.fori_loop(0, rows // TQ, turn, 0)


def forward_near(q0, qa, qb, l0, l1, la, lb, lc, ld, ku, vu, qp, do, qtag, compt, kp, kpt, v, ktag, stats):
    blocks = [q0[i] for i in range(4)] + [qb[i] for i in range(4)] + [qa[i] for i in range(4)]
    take_queries(blocks, qp, do, qtag)
    keys = [l0[...], l1[...], lb[0], lb[1], lc[0], ld[0], la[0], la[1]]
    for n, block in enumerate(keys):
        at = 128 * n
        compt[:, at : at + 128] = block[0:512]
        kpt[128:192, at : at + 128] = block[512:576]
        ktag[8 * n : 8 * n + 8] = block[576:592].astype(F32)[0:8]
    kpt[192:256] = jnp.zeros((64, NK), BF)
    kpt[0:128] = mm(ku[...].T, compt[...], NN).astype(BF)
    v[...] = mm(vu[...].T, compt[...], NN).astype(BF).T
    kp[...] = kpt[...].T
    stats[...] = jnp.zeros_like(stats)
    statistics(1536, qp, do, qtag, kp, v, ktag, stats, 0)


def forward_far(qc, qd, kp, v, ktag, near, qp, do, qtag, stats):
    take_queries([qc[0], qc[1], qd[0], qd[1]], qp, do, qtag)
    stats[:, 0:1536] = near[...]
    stats[:, 1536:2048] = jnp.zeros((8, 512), F32)
    statistics(512, qp, do, qtag, kp, v, ktag, stats, 1536)


START = {0: 0, 1: 512, 3: 1024, 2: 1536}


def backward(z, qp, do, qtag, qp2, do2, qtag2, compt, kp, kpt, v, ktag, s0, s1, s2, s3, *rest):
    zpay, xpay, (dk, dv, low, up) = rest[:4], rest[4:8], rest[8:]
    late = lateness()
    ktags = [ktag[8 * n : 8 * n + 1] for n in range(8)]
    stats = [s0, s1, s2, s3]
    for r in range(4):
        rows = []
        for d in range(4):
            at = START[(r - d) % 4]
            rows.append([stats[d][n : n + 1, at : at + 512] for n in range(3)])
        top = functools.reduce(jnp.maximum, [t[0] for t in rows])
        total = sum(t[1] * jnp.exp2(t[0] - top) for t in rows)
        weighted = sum(t[2] * jnp.exp2(t[0] - top) for t in rows)
        at = START[r]
        low[0:1, at : at + 512] = top + jnp.log2(total)
        low[1:2, at : at + 512] = weighted / total
    dk[...] = jnp.zeros_like(dk)
    dv[...] = jnp.zeros_like(dv)
    for r in (0, 1, 3, 2):
        for i in range(2):
            to = START[r] + i * TQ
            if r == 2:
                q, g, qt = qp2[i * TQ : i * TQ + TQ], do2[i * TQ : i * TQ + TQ], qtag2[0:1, i * TQ : i * TQ + TQ]
            else:
                q, g, qt = qp[to : to + TQ], do[to : to + TQ], qtag[0:1, to : to + TQ]
            raw = mm(kp[...], q, NT)
            s = masked_scores(raw, [qt[:, 0:128], qt[:, 128:256]], ktags, late)
            p = jnp.exp2(s - low[0:1, to : to + TQ])
            dp = mm(v[...], g, NT)
            ds = (p * (dp - low[1:2, to : to + TQ])).astype(BF)
            dk[...] += mm(ds, q, NN)
            dv[...] += mm(p.astype(BF), g, NN)
            dq = (mm(kpt[...], ds, NN).T * SCALE).astype(BF)
            for b in range(2):
                m = 2 * i + b
                zpay[r][128 * m : 128 * m + 128] = dq[128 * b : 128 * b + 128, 0:128]
                zpay[r][512 + 64 * m : 576 + 64 * m] = dense_rope(dq[128 * b : 128 * b + 128, 128:192])
    dk16 = (dk[...] * SCALE).astype(BF)
    dv16 = dv[...].astype(BF)
    drope = dk16[:, 128:256].T
    for n in range(8):
        r, m = n // 2, n % 2
        xpay[r][128 * m : 128 * m + 128] = dk16[128 * n : 128 * n + 128, 0:128]
        xpay[r][256 + 128 * m : 384 + 128 * m] = dv16[128 * n : 128 * n + 128]
        xpay[r][512 + 64 * m : 576 + 64 * m] = drope[0:64, 128 * n : 128 * n + 128]
    up[...] = mm(compt[...], jnp.concatenate([dk16[:, 0:128], dv16], axis=1), NN).astype(BF)
    for r in range(4):
        at = pl.multiple_of(lax.rem(z[0] + r, 4) * 128, 128)
        part = up[pl.ds(at, 128)]
        zpay[r][768:896] = part[:, 0:128]
        zpay[r][896:1024] = part[:, 128:256]


def middle(xy, z0, z1, z2, z3, x0, x1, x2, x3, ku, vu, pay, lat, upk, qback, up):
    def total(rows):
        return sum(a[rows].astype(F32) for a in (z0, z1, z2, z3))

    for h in range(4):
        qback[h, 0:128] = total(slice(128 * h, 128 * h + 128)).astype(BF)
        qback[h, 128:192] = total(slice(512 + 64 * h, 576 + 64 * h)).astype(BF)
    up[...] = total(slice(768, 1024))
    keep = pl.multiple_of(xy[1] * 64, 64)
    give = pl.multiple_of((1 - xy[1]) * 64, 64)
    for n in range(2):
        upk[64 * n : 64 * n + 64] = up[pl.ds(128 * n + keep, 64)]
        pay[576 + 64 * n : 640 + 64 * n] = up[pl.ds(128 * n + give, 64)].astype(BF)
    acc = jnp.zeros((512, 256), F32)
    rope = jnp.zeros((128, 128), F32)
    for r, p in enumerate((x0, x1, x2, x3)):
        h = pl.multiple_of(lax.rem(xy[0] + 4 - r, 4) * 128, 128)
        acc += mm(ku[:, pl.ds(h, 128)], p[0:256], NT)
        acc += mm(vu[:, pl.ds(h, 128)], p[256:512], NT)
        rope += p[512:640].astype(F32)
    lat[0:512] = acc[:, 0:128]
    lat[512:576] = rope[0:64]
    pay[0:512] = acc[:, 128:256].astype(BF)
    pay[512:576] = rope[64:128].astype(BF)


def spread(got, lat, upk, lat16, every):
    lat16[...] = (lat[...] + got[0:576].astype(F32)).astype(BF)
    mine = (upk[...] + got[576:704].astype(F32)).astype(BF)
    for n in range(32):
        every[n] = mine


def unpack_query_grad(a, out):
    for h in range(4):
        out[:, 192 * h : 192 * h + 128] = a[h, 0:128]
        out[:, 192 * h + 128 : 192 * h + 192] = wide_rope(a[h, 128:192])


def unpack_up(a, key, value):
    for y in range(2):
        for z in range(4):
            for x in range(4):
                part = a[place(y, z, x)].astype(F32)
                at = 128 * z + 64 * y
                key[at : at + 64, 128 * x : 128 * x + 128] = part[0:64]
                value[at : at + 64, 128 * x : 128 * x + 128] = part[64:128]


def shards(queries, latents, key_up, value_up, out_grad, positions):
    here = lax.axis_index("seq").astype(jnp.int32)
    y, z, x = here >> 4, (here >> 2) & 3, here & 3
    stripe = lax.shift_right_logical(positions[0:1], 7)
    lat = jnp.concatenate([latents.T, jnp.broadcast_to(stripe.astype(BF)[:, None], (16, 128))], axis=0)
    lat_y = along(lat, dy=1)
    (qpk,) = call(pack_queries, [((4, QP, 128), BF)], stripe, queries, out_grad, smem=1, name="pack_queries")
    ku = lax.dynamic_slice(key_up, (0, x * 128), (D_LAT, 128))
    vu = lax.dynamic_slice(value_up, (0, x * 128), (D_LAT, 128))

    q0 = lax.all_to_all(qpk, "seq", 0, 0, tiled=True, axis_index_groups=X_GROUPS)
    qa = along(q0, dz=1)
    qb = along(q0, dz=-1)
    pair = jnp.stack([lat, lat_y])
    la = along(pair, dx=1)
    lb = along(pair, dx=-1)
    qc = along(qa[:2], dz=1)
    qd = along(qb[2:], dz=-1)
    lc = along(la[:1], dx=1)
    ld = along(lb[1:], dx=-1)

    flops = 2 * NQ * NK * 512
    outs = [
        ((1536, 256), BF), ((1536, 128), BF), ((8, 1536), F32), ((512, NK), BF), ((NK, 256), BF),
        ((256, NK), BF), ((NK, 128), BF), ((64, 128), F32), ((8, 1536), F32),
    ]
    *near, stats = call(
        forward_near, outs, q0, qa, qb, lat, lat_y, la, lb, lc, ld, ku, vu,
        flops=flops * 3 // 4, grant=20, name="forward_near",
    )
    qp, do, qtag, compt, kp, kpt, v, ktag = near
    outs = [((512, 256), BF), ((512, 128), BF), ((8, 512), F32), ((8, NQ), F32)]
    *far, stats = call(
        forward_far, outs, qc, qd, kp, v, ktag, stats, flops=flops // 4, grant=12, name="forward_far"
    )
    s3 = along(stats, dz=1)
    s1 = along(stats, dz=-1)
    s2 = along(stats, dz=2)

    pays = call(
        backward,
        [((1024, 128), BF)] * 4 + [((640, 128), BF)] * 4,
        z[None], qp, do, qtag, *far, compt, kp, kpt, v, ktag, stats, s1, s2, s3,
        scratch=[
            pltpu.VMEM((NK, 256), F32), pltpu.VMEM((NK, 128), F32),
            pltpu.VMEM((8, NQ), F32), pltpu.VMEM((512, 256), BF),
        ],
        smem=1, flops=3 * flops, grant=24, name="backward",
    )
    zpay, xpay = pays[:4], pays[4:]
    xr = [along(xpay[r], dx=r) for r in (1, 2, 3)]
    zr = [along(zpay[r], dz=r) for r in (1, 2, 3)]
    pay, mine, upk, qback = call(
        middle,
        [((704, 128), BF), ((576, 128), F32), ((128, 128), F32), ((4, 192, 128), BF)],
        jnp.stack([x, y]), zpay[0], *zr, xpay[0], *xr, key_up, value_up,
        scratch=[pltpu.VMEM((256, 128), F32)], smem=1, flops=2 * 256 * 512 * 1024, grant=10, name="middle",
    )
    got = along(pay, dy=1)
    qhome = lax.all_to_all(qback, "seq", 0, 0, tiled=True, axis_index_groups=X_GROUPS)
    lat16, every = call(spread, [((576, 128), BF), ((32, 128, 128), BF)], got, mine, upk, name="spread")
    whole = lax.all_to_all(every, "seq", 0, 0, tiled=True)
    near16 = lax.ppermute(lat16, "head", [(0, 1), (1, 0), (2, 3), (3, 2)])
    two = lax.reduce_precision(lat16.astype(F32) + near16.astype(F32), 8, 7).astype(BF)
    far16 = lax.ppermute(two, "head", [(0, 2), (1, 3), (2, 0), (3, 1)])
    latent_grad = (two.astype(F32) + far16.astype(F32)).T
    (query_grad,) = call(unpack_query_grad, [((ROWS, 768), BF)], qhome, name="unpack_query_grad")
    key_up_grad, value_up_grad = call(
        unpack_up, [((512, 512), F32), ((512, 512), F32)], whole, name="unpack_up"
    )
    return (query_grad, latent_grad, key_up_grad, value_up_grad)


def solution(mesh):
    in_specs = (
        P("seq", "head"),
        P("seq", None),
        P(None, "head"),
        P(None, "head"),
        P("seq", "head"),
        P("seq"),
    )
    out_specs = (P("seq", "head"), P("seq", None), P(None, "head"), P(None, "head"))
    return jax.shard_map(shards, mesh=mesh, in_specs=in_specs, out_specs=out_specs, check_vma=False)
```

```python
import functools
import math

import jax
import jax.numpy as jnp
from jax import lax
from jax.experimental import pallas as pl
from jax.experimental.pallas import tpu as pltpu
from jax.sharding import PartitionSpec as P

BF = jnp.bfloat16
F32 = jnp.float32
D_LAT = 512
D_ROPE = 64
D_NOPE = 128
D_V = 128
ROWS = 128
SCALE = 1.0 / math.sqrt(D_NOPE + D_ROPE)
SCALE2 = SCALE * math.log2(math.e)
NEG = -1e30
QP = 336
LP = 592
NQ = 2048
NK = 1024
TQ = 256


def place(y, z, x):
    return (y % 2) * 16 + (z % 4) * 4 + x % 4


def along(value, dy=0, dz=0, dx=0):
    pairs = [
        (place(y, z, x), place(y + dy, z + dz, x + dx))
        for y in range(2)
        for z in range(4)
        for x in range(4)
    ]
    return lax.ppermute(value, "seq", pairs)


VM, SM, HB = pltpu.VMEM, pltpu.SMEM, pltpu.HBM


def call(kernel, outs, args, scratch=(), flops=0, grant=6, name=None):
    args = [arg if isinstance(arg, tuple) else (arg, VM) for arg in args]
    args = [(pltpu.with_memory_space_constraint(a, HB) if m is HB else a, m) for a, m in args]
    return pl.pallas_call(
        kernel,
        out_shape=[HB(o[0], o[1]) if o[2:] == (HB,) else jax.ShapeDtypeStruct(o[0], o[1]) for o in outs],
        in_specs=[pl.BlockSpec(memory_space=space) for _, space in args],
        out_specs=[pl.BlockSpec(memory_space=o[2] if len(o) > 2 else VM) for o in outs],
        scratch_shapes=list(scratch),
        cost_estimate=pl.CostEstimate(flops=max(flops, 1), bytes_accessed=1 << 20, transcendentals=0),
        compiler_params=pltpu.CompilerParams(vmem_limit_bytes=grant << 20),
        name=name,
    )(*[array for array, _ in args])


def dense_rope(block):
    return jnp.concatenate([block[0:64], block[64:128]], axis=1)


def wide_rope(block):
    return jnp.concatenate([block[:, 0:64], block[:, 64:128]], axis=0)


def pack(pos, x, q_hbm, g_hbm, lat_hbm, own, to1, to2, to3, lat, q, g, heads, sems):
    copies = [
        pltpu.make_async_copy(q_hbm, q, sems.at[0]),
        pltpu.make_async_copy(g_hbm, g, sems.at[1]),
        pltpu.make_async_copy(lat_hbm, lat.at[0:576], sems.at[2]),
    ]
    for copy in copies:
        copy.start()
    tag = jnp.full((16, 128), (pos[0] >> 7).astype(F32), F32).astype(BF)
    lat[576:592] = tag
    for copy in copies:
        copy.wait()
    for h in range(4):
        heads[h, 0:128] = q[:, 192 * h : 192 * h + 128]
        heads[h, 128:256] = g[:, 128 * h : 128 * h + 128]
        heads[h, 256:320] = dense_rope(q[:, 192 * h + 128 : 192 * h + 192])
        heads[h, 320:336] = tag
    for r, out in enumerate((own, to1, to2, to3)):
        out[...] = heads[(x[0] + r) & 3]


def masked_scores(raw, qtags, ktags, late):
    rows = []
    for kb in range(NK // 128):
        cols = []
        for qb in range(TQ // 128):
            part = raw[128 * kb : 128 * kb + 128, 128 * qb : 128 * qb + 128]
            seen = late <= (qtags[qb] - ktags[kb]) * 128.0
            cols.append(jnp.where(seen, part * SCALE2, NEG))
        rows.append(jnp.concatenate(cols, axis=1))
    return jnp.concatenate(rows, axis=0)


def lateness():
    shape = (128, 128)
    return (lax.broadcasted_iota(jnp.int32, shape, 0) - lax.broadcasted_iota(jnp.int32, shape, 1)).astype(F32)


NT = (((1,), (1,)), ((), ()))
NN = (((1,), (0,)), ((), ()))


def mm(a, b, dims):
    return lax.dot_general(a, b, dims, preferred_element_type=F32)


def take_queries(blocks, qp, do, qtag):
    zeros = jnp.zeros((128, 64), BF)
    for n, block in enumerate(blocks):
        at = 128 * n
        qp[at : at + 128, 0:128] = block[0:128]
        qp[at : at + 128, 128:256] = jnp.concatenate([wide_rope(block[256:320]), zeros], axis=1)
        do[at : at + 128] = block[128:256]
        qtag[0:8, at : at + 128] = block[320:336].astype(F32)[0:8]


def statistics(rows, qp, do, qtag, kp, v, ktag, stats, first):
    late = lateness()
    ktags = [ktag[8 * n : 8 * n + 1] for n in range(8)]

    def turn(i, carry):
        at = pl.multiple_of(i * TQ, TQ)
        to = pl.multiple_of(first + i * TQ, TQ)
        raw = mm(kp[...], qp[pl.ds(at, TQ)], NT)
        qt = qtag[0:1, pl.ds(at, TQ)]
        s = masked_scores(raw, [qt[:, 0:128], qt[:, 128:256]], ktags, late)
        top = jnp.max(s, axis=0, keepdims=True)
        p = jnp.exp2(s - top)
        dp = mm(v[...], do[pl.ds(at, TQ)], NT)
        stats[0:1, pl.ds(to, TQ)] = top
        stats[1:2, pl.ds(to, TQ)] = jnp.sum(p, axis=0, keepdims=True)
        stats[2:3, pl.ds(to, TQ)] = jnp.sum(p * dp, axis=0, keepdims=True)
        return carry

    lax.fori_loop(0, rows // TQ, turn, 0)


def copied(pairs, sems):
    copies = [pltpu.make_async_copy(src, dst, sems.at[n]) for n, (src, dst) in enumerate(pairs)]
    for copy in copies:
        copy.start()
    return copies


def forward_near(
    q0, q1, a0, a1, b0, b1, l0, l1, la0, la1, lb0, lb1, lc, ld, ku, vu,
    qp_hbm, do_hbm, compt_hbm, kpt_hbm, qtag_hbm, kp_hbm, v_hbm, ktag_hbm, kp, v, ktag, stats,
    qp, do, compt, kpt, qtag, sems, late_sems,
):
    take_queries([ref[i] for ref in (q0, q1, b0, b1, a0, a1) for i in range(2)], qp, do, qtag)
    keys = [l0, l1, lb0, lb1, lc, ld, la0, la1]
    for n, block in enumerate(keys):
        at = 128 * n
        compt[:, at : at + 128] = block[0:512]
        kpt[128:192, at : at + 128] = block[512:576]
        ktag[8 * n : 8 * n + 8] = block[576:592].astype(F32)[0:8]
    kpt[192:256] = jnp.zeros((64, NK), BF)
    kpt[0:128] = mm(ku[...].T, compt[...], NN).astype(BF)
    pairs = [(qp, qp_hbm), (do, do_hbm), (compt, compt_hbm), (kpt, kpt_hbm), (qtag, qtag_hbm), (ktag, ktag_hbm)]
    copies = copied(pairs, sems)
    v[...] = mm(vu[...].T, compt[...], NN).astype(BF).T
    kp[...] = kpt[...].T
    copies += copied([(kp, kp_hbm), (v, v_hbm)], late_sems)
    stats[...] = jnp.zeros_like(stats)
    statistics(1536, qp, do, qtag, kp, v, ktag, stats, 0)
    for copy in copies:
        copy.wait()


def forward_far(qc, qd, kp, v, ktag, near, qp_hbm, do_hbm, qtag_hbm, stats, qp, do, qtag, sems):
    take_queries([qc[0], qc[1], qd[0], qd[1]], qp, do, qtag)
    copies = copied([(qp, qp_hbm), (do, do_hbm), (qtag, qtag_hbm)], sems)
    stats[:, 0:1536] = near[...]
    stats[:, 1536:2048] = jnp.zeros((8, 512), F32)
    statistics(512, qp, do, qtag, kp, v, ktag, stats, 1536)
    for copy in copies:
        copy.wait()


START = {0: 0, 1: 512, 3: 1024, 2: 1536}


def backward(z, *refs):
    there, (s0, s1, s2, s3), zpay, xpay, (dk, dv, low, up) = refs[:11], refs[11:15], refs[15:19], refs[19:23], refs[23:27]
    here, sems = refs[27:38], refs[38]
    kp, ktag, qp, qtag, v, do, kpt, qp2, qtag2, do2, compt = here
    copies = copied(list(zip(there, here)), sems)
    copies[1].wait()
    late = lateness()
    ktags = [ktag[8 * n : 8 * n + 1] for n in range(8)]
    stats = [s0, s1, s2, s3]
    for r in range(4):
        rows = []
        for d in range(4):
            at = START[(r - d) % 4]
            rows.append([stats[d][n : n + 1, at : at + 512] for n in range(3)])
        top = functools.reduce(jnp.maximum, [t[0] for t in rows])
        total = sum(t[1] * jnp.exp2(t[0] - top) for t in rows)
        weighted = sum(t[2] * jnp.exp2(t[0] - top) for t in rows)
        at = START[r]
        low[0:1, at : at + 512] = top + jnp.log2(total)
        low[1:2, at : at + 512] = weighted / total
    dk[...] = jnp.zeros_like(dk)
    dv[...] = jnp.zeros_like(dv)
    for n in (0, 2, 3, 4, 5, 6):
        copies[n].wait()
    for r in (0, 1, 3, 2):
        if r == 2:
            for copy in copies[7:10]:
                copy.wait()
        for i in range(2):
            to = START[r] + i * TQ
            if r == 2:
                q, g, qt = qp2[i * TQ : i * TQ + TQ], do2[i * TQ : i * TQ + TQ], qtag2[0:1, i * TQ : i * TQ + TQ]
            else:
                q, g, qt = qp[to : to + TQ], do[to : to + TQ], qtag[0:1, to : to + TQ]
            raw = mm(kp[...], q, NT)
            s = masked_scores(raw, [qt[:, 0:128], qt[:, 128:256]], ktags, late)
            p = jnp.exp2(s - low[0:1, to : to + TQ])
            dp = mm(v[...], g, NT)
            ds = (p * (dp - low[1:2, to : to + TQ])).astype(BF)
            dk[...] += mm(ds, q, NN)
            dv[...] += mm(p.astype(BF), g, NN)
            dq = (mm(kpt[...], ds, NN).T * SCALE).astype(BF)
            for b in range(2):
                m = 2 * i + b
                zpay[r][128 * m : 128 * m + 128] = dq[128 * b : 128 * b + 128, 0:128]
                zpay[r][512 + 64 * m : 576 + 64 * m] = dense_rope(dq[128 * b : 128 * b + 128, 128:192])
    dk16 = (dk[...] * SCALE).astype(BF)
    dv16 = dv[...].astype(BF)
    drope = dk16[:, 128:256].T
    for n in range(8):
        r, m = n // 2, n % 2
        xpay[r][128 * m : 128 * m + 128] = dk16[128 * n : 128 * n + 128, 0:128]
        xpay[r][256 + 128 * m : 384 + 128 * m] = dv16[128 * n : 128 * n + 128]
        xpay[r][512 + 64 * m : 576 + 64 * m] = drope[0:64, 128 * n : 128 * n + 128]
    copies[10].wait()
    up[...] = mm(compt[...], jnp.concatenate([dk16[:, 0:128], dv16], axis=1), NN).astype(BF)
    for r in range(4):
        at = pl.multiple_of(lax.rem(z[0] + r, 4) * 128, 128)
        part = up[pl.ds(at, 128)]
        zpay[r][768:896] = part[:, 0:128]
        zpay[r][896:1024] = part[:, 128:256]


def middle(xy, z0, z1, z2, z3, x0, x1, x2, x3, ku, vu, pay, lat, upk, q0, q1, q2, q3, up):
    def total(rows):
        return sum(a[rows].astype(F32) for a in (z0, z1, z2, z3))

    for r, back in enumerate((q0, q1, q2, q3)):
        back[0:128] = total(slice(128 * r, 128 * r + 128)).astype(BF)
        back[128:192] = total(slice(512 + 64 * r, 576 + 64 * r)).astype(BF)
    up[...] = total(slice(768, 1024))
    keep = pl.multiple_of(xy[1] * 64, 64)
    give = pl.multiple_of((1 - xy[1]) * 64, 64)
    for n in range(2):
        upk[64 * n : 64 * n + 64] = up[pl.ds(128 * n + keep, 64)]
        pay[576 + 64 * n : 640 + 64 * n] = up[pl.ds(128 * n + give, 64)].astype(BF)
    acc = jnp.zeros((512, 256), F32)
    rope = jnp.zeros((128, 128), F32)
    for r, p in enumerate((x0, x1, x2, x3)):
        h = pl.multiple_of(lax.rem(xy[0] + 4 - r, 4) * 128, 128)
        acc += mm(ku[:, pl.ds(h, 128)], p[0:256], NT)
        acc += mm(vu[:, pl.ds(h, 128)], p[256:512], NT)
        rope += p[512:640].astype(F32)
    lat[0:512] = acc[:, 0:128]
    lat[512:576] = rope[0:64]
    pay[0:512] = acc[:, 128:256].astype(BF)
    pay[512:576] = rope[64:128].astype(BF)


def spread(got, lat, upk, lat16, every):
    lat16[...] = (lat[...] + got[0:576].astype(F32)).astype(BF)
    mine = (upk[...] + got[576:704].astype(F32)).astype(BF)
    for n in range(32):
        every[n] = mine


def unpack_query_grad(x, q0, q1, q2, q3, out, heads):
    for r, ref in enumerate((q0, q1, q2, q3)):
        heads[(x[0] + r) & 3] = ref[...]
    for h in range(4):
        out[:, 192 * h : 192 * h + 128] = heads[h, 0:128]
        out[:, 192 * h + 128 : 192 * h + 192] = wide_rope(heads[h, 128:192])


def unpack_up(a, key, value):
    for y in range(2):
        for z in range(4):
            for x in range(4):
                part = a[place(y, z, x)].astype(F32)
                at = 128 * z + 64 * y
                key[at : at + 64, 128 * x : 128 * x + 128] = part[0:64]
                value[at : at + 64, 128 * x : 128 * x + 128] = part[64:128]


def shards(queries, latents, key_up, value_up, out_grad, positions):
    here = lax.axis_index("seq").astype(jnp.int32)
    y, z, x = here >> 4, (here >> 2) & 3, here & 3
    part = ((QP, 128), BF)
    own, to1, to2, to3, lat = call(
        pack,
        [part, part, part, part, ((LP, 128), BF)],
        [(positions, SM), (x[None], SM), (queries, HB), (out_grad, HB), (latents.T, HB)],
        scratch=[
            pltpu.VMEM((ROWS, 768), BF), pltpu.VMEM((ROWS, 512), BF), pltpu.VMEM((4, QP, 128), BF),
            pltpu.SemaphoreType.DMA((3,)),
        ],
        name="pack",
    )
    q_1 = along(to1, dx=1)
    q_3 = along(to3, dx=-1)
    lat_y = along(lat, dy=1)
    q_2 = along(to2, dx=2)
    la0 = along(lat, dx=1)
    lb0 = along(lat, dx=-1)
    q0 = jnp.stack([own, q_1])
    q1 = jnp.stack([q_2, q_3])
    ku = lax.dynamic_slice(key_up, (0, x * 128), (D_LAT, 128))
    vu = lax.dynamic_slice(value_up, (0, x * 128), (D_LAT, 128))

    qa0, qb0 = along(q0, dz=1), along(q0, dz=-1)
    qa1, qb1 = along(q1, dz=1), along(q1, dz=-1)
    la1 = along(lat_y, dx=1)
    lb1 = along(lat_y, dx=-1)
    qc = along(qa0, dz=1)
    qd = along(qb1, dz=-1)
    lc = along(la0, dx=1)
    ld = along(lb1, dx=-1)

    flops = 2 * NQ * NK * 512
    near = [
        ((1536, 256), BF), ((1536, 128), BF), ((512, NK), BF), ((256, NK), BF), ((8, 1536), F32),
        ((NK, 256), BF), ((NK, 128), BF), ((64, 128), F32),
    ]
    qp, do, compt, kpt, qtag, kp, v, ktag, kp_here, v_here, ktag_here, stats = call(
        forward_near,
        [(*o, HB) for o in near] + near[5:8] + [((8, 1536), F32)],
        [q0, q1, qa0, qa1, qb0, qb1, lat, lat_y, la0, la1, lb0, lb1, lc, ld, ku, vu],
        scratch=[pltpu.VMEM(*o) for o in near[:5]] + [pltpu.SemaphoreType.DMA((6,)), pltpu.SemaphoreType.DMA((2,))],
        flops=flops * 3 // 4, grant=20, name="forward_near",
    )
    far = [((512, 256), BF), ((512, 128), BF), ((8, 512), F32)]
    qp2, do2, qtag2, stats = call(
        forward_far,
        [(*o, HB) for o in far] + [((8, NQ), F32)],
        [qc, qd, kp_here, v_here, ktag_here, stats],
        scratch=[pltpu.VMEM(*o) for o in far] + [pltpu.SemaphoreType.DMA((3,))],
        flops=flops // 4, grant=12, name="forward_far",
    )
    s3 = along(stats, dz=1)
    s1 = along(stats, dz=-1)
    s2 = along(stats, dz=2)

    there = [kp, ktag, qp, qtag, v, do, kpt, qp2, qtag2, do2, compt]
    pays = call(
        backward,
        [((1024, 128), BF)] * 4 + [((640, 128), BF)] * 4,
        [(z[None], SM)] + [(a, HB) for a in there] + [stats, s1, s2, s3],
        scratch=[
            pltpu.VMEM((NK, 256), F32), pltpu.VMEM((NK, 128), F32),
            pltpu.VMEM((8, NQ), F32), pltpu.VMEM((512, 256), BF),
            *[pltpu.VMEM(a.shape, a.dtype) for a in there], pltpu.SemaphoreType.DMA((11,)),
        ],
        flops=3 * flops, grant=24, name="backward",
    )
    zpay, xpay = pays[:4], pays[4:]
    x1, x3 = along(xpay[1], dx=1), along(xpay[3], dx=3)
    z1, z3 = along(zpay[1], dz=1), along(zpay[3], dz=3)
    x2 = along(xpay[2], dx=2)
    z2 = along(zpay[2], dz=2)
    back = ((192, 128), BF)
    pay, mine, upk, b0, b1, b2, b3 = call(
        middle,
        [((704, 128), BF), ((576, 128), F32), ((128, 128), F32), back, back, back, back],
        [(jnp.stack([x, y]), SM), zpay[0], z1, z2, z3, xpay[0], x1, x2, x3, key_up, value_up],
        scratch=[pltpu.VMEM((256, 128), F32)], flops=2 * 256 * 512 * 1024, grant=10, name="middle",
    )
    got = along(pay, dy=1)
    c1, c3 = along(b1, dx=-1), along(b3, dx=-3)
    c2 = along(b2, dx=-2)
    lat16, every = call(spread, [((576, 128), BF), ((32, 128, 128), BF)], [got, mine, upk], name="spread")
    whole = lax.all_to_all(every, "seq", 0, 0, tiled=True)
    near16 = lax.ppermute(lat16, "head", [(0, 1), (1, 0), (2, 3), (3, 2)])
    two = lax.reduce_precision(lat16.astype(F32) + near16.astype(F32), 8, 7).astype(BF)
    far16 = lax.ppermute(two, "head", [(0, 2), (1, 3), (2, 0), (3, 1)])
    latent_grad = (two.astype(F32) + far16.astype(F32)).T
    (query_grad,) = call(
        unpack_query_grad, [((ROWS, 768), BF)], [(x[None], SM), b0, c1, c2, c3],
        scratch=[pltpu.VMEM((4, 192, 128), BF)], name="unpack_query_grad",
    )
    key_up_grad, value_up_grad = call(
        unpack_up, [((512, 512), F32), ((512, 512), F32)], [whole], name="unpack_up"
    )
    return (query_grad, latent_grad, key_up_grad, value_up_grad)


def solution(mesh):
    in_specs = (
        P("seq", "head"),
        P("seq", None),
        P(None, "head"),
        P(None, "head"),
        P("seq", "head"),
        P("seq"),
    )
    out_specs = (P("seq", "head"), P("seq", None), P(None, "head"), P(None, "head"))
    return jax.shard_map(shards, mesh=mesh, in_specs=in_specs, out_specs=out_specs, check_vma=False)
```

```python
import functools
import math

import jax
import jax.numpy as jnp
from jax import lax
from jax.experimental import pallas as pl
from jax.experimental.pallas import tpu as pltpu
from jax.sharding import PartitionSpec as P


BF = jnp.bfloat16
F32 = jnp.float32
D_LAT = 512
D_ROPE = 64
D_NOPE = 128
ROWS = 128
SCALE = 1.0 / math.sqrt(D_NOPE + D_ROPE)
SCALE2 = SCALE * math.log2(math.e)
NEG = -1e30
QP = 336
LP = 592
NQ = 2048
NK = 1024
TQ = 256


def place(y, z, x):
    return (y % 2) * 16 + (z % 4) * 4 + x % 4


def along(value, dy=0, dz=0, dx=0):
    pairs = [
        (place(y, z, x), place(y + dy, z + dz, x + dx))
        for y in range(2)
        for z in range(4)
        for x in range(4)
    ]
    return lax.ppermute(value, "seq", pairs)


def by_core(value, dx):
    pairs = []
    for y in range(2):
        for z in range(4):
            for x in range(4):
                for h in range(4):
                    step = dx if h % 2 == 0 else -dx
                    pairs.append((place(y, z, x) * 4 + h, place(y, z, x + step) * 4 + h))
    return lax.ppermute(value, ("seq", "head"), pairs)


def to_core(value):
    return lax.ppermute(value, "head", [(0, 1), (1, 0), (2, 3), (3, 2)])


YZ_GROUPS = [[4 * k + i for k in range(8)] for i in range(4)]
VM, SM, HB = pltpu.VMEM, pltpu.SMEM, pltpu.HBM


def call(kernel, outs, args, scratch=(), flops=0, grant=6):
    args = [arg if isinstance(arg, tuple) else (arg, VM) for arg in args]
    args = [(pltpu.with_memory_space_constraint(a, HB) if m is HB else a, m) for a, m in args]
    return pl.pallas_call(
        kernel,
        out_shape=[HB(o[0], o[1]) if o[2:] == (HB,) else jax.ShapeDtypeStruct(o[0], o[1]) for o in outs],
        in_specs=[pl.BlockSpec(memory_space=space) for _, space in args],
        out_specs=[pl.BlockSpec(memory_space=o[2] if len(o) > 2 else VM) for o in outs],
        scratch_shapes=list(scratch),
        cost_estimate=pl.CostEstimate(flops=max(flops, 1), bytes_accessed=1 << 20, transcendentals=0),
        compiler_params=pltpu.CompilerParams(vmem_limit_bytes=grant << 20),
    )(*[array for array, _ in args])


def dense_rope(block):
    return jnp.concatenate([block[0:64], block[64:128]], axis=1)


def wide_rope(block):
    return jnp.concatenate([block[:, 0:64], block[:, 64:128]], axis=0)


def pack(pos_hbm, x, q_hbm, g_hbm, lat_hbm, own, to1, to2, to3, lat, q, g, heads, pos, sems):
    copies = [
        pltpu.make_async_copy(q_hbm, q, sems.at[0]),
        pltpu.make_async_copy(g_hbm, g, sems.at[1]),
        pltpu.make_async_copy(lat_hbm, lat.at[0:576], sems.at[2]),
        pltpu.make_async_copy(pos_hbm, pos, sems.at[3]),
    ]
    for copy in copies:
        copy.start()
    copies.pop().wait()
    tag = jnp.full((16, 128), (pos[0] >> 7).astype(F32), F32).astype(BF)
    lat[576:592] = tag
    for copy in copies:
        copy.wait()
    for h in range(4):
        heads[h, 0:128] = q[:, 192 * h : 192 * h + 128]
        heads[h, 128:256] = g[:, 128 * h : 128 * h + 128]
        heads[h, 256:320] = dense_rope(q[:, 192 * h + 128 : 192 * h + 192])
        heads[h, 320:336] = tag
    for r, out in enumerate((own, to1, to2, to3)):
        out[...] = heads[(x[0] + r) & 3]


def masked_scores(raw, qtags, ktags, late):
    rows = []
    for kb in range(NK // 128):
        cols = []
        for qb in range(TQ // 128):
            part = raw[128 * kb : 128 * kb + 128, 128 * qb : 128 * qb + 128]
            seen = late <= (qtags[qb] - ktags[kb]) * 128.0
            cols.append(jnp.where(seen, part * SCALE2, NEG))
        rows.append(jnp.concatenate(cols, axis=1))
    return jnp.concatenate(rows, axis=0)


def lateness():
    shape = (128, 128)
    return (lax.broadcasted_iota(jnp.int32, shape, 0) - lax.broadcasted_iota(jnp.int32, shape, 1)).astype(F32)


NT = (((1,), (1,)), ((), ()))
NN = (((1,), (0,)), ((), ()))


def mm(a, b, dims):
    return lax.dot_general(a, b, dims, preferred_element_type=F32)


def take_queries(blocks, qp, do, qtag):
    zeros = jnp.zeros((128, 64), BF)
    for n, block in enumerate(blocks):
        at = 128 * n
        qp[at : at + 128, 0:128] = block[0:128]
        qp[at : at + 128, 128:256] = jnp.concatenate([wide_rope(block[256:320]), zeros], axis=1)
        do[at : at + 128] = block[128:256]
        qtag[0:8, at : at + 128] = block[320:336].astype(F32)[0:8]


def statistics(rows, qp, do, qtag, kp, v, ktag, stats, first):
    late = lateness()
    ktags = [ktag[8 * n : 8 * n + 1] for n in range(8)]

    def turn(i, carry):
        at = pl.multiple_of(i * TQ, TQ)
        to = pl.multiple_of(first + i * TQ, TQ)
        raw = mm(kp[...], qp[pl.ds(at, TQ)], NT)
        qt = qtag[0:1, pl.ds(at, TQ)]
        s = masked_scores(raw, [qt[:, 0:128], qt[:, 128:256]], ktags, late)
        top = jnp.max(s, axis=0, keepdims=True)
        p = jnp.exp2(s - top)
        dp = mm(v[...], do[pl.ds(at, TQ)], NT)
        stats[0:1, pl.ds(to, TQ)] = top
        stats[1:2, pl.ds(to, TQ)] = jnp.sum(p, axis=0, keepdims=True)
        stats[2:3, pl.ds(to, TQ)] = jnp.sum(p * dp, axis=0, keepdims=True)
        return carry

    lax.fori_loop(0, rows // TQ, turn, 0)


def copied(pairs, sems):
    copies = [pltpu.make_async_copy(src, dst, sems.at[n]) for n, (src, dst) in enumerate(pairs)]
    for copy in copies:
        copy.start()
    return copies


def forward_near(
    core, q0, qa, qb, pair, lp, lpe, lh, lhe, ku, vu,
    qp_hbm, do_hbm, compt_hbm, kpt_hbm, qtag_hbm, kp_hbm, v_hbm, ktag_hbm, kp, v, ktag, stats,
    qp, do, compt, kpt, qtag, sems, late_sems,
):
    take_queries([ref[i] for ref in (q0, qb, qa) for i in range(4)], qp, do, qtag)
    first = core[0] == 0
    for n in range(8):
        if n < 2:
            block = pair[n]
        elif n in (4, 5):
            mine, other = (lh, lhe) if n == 4 else (lhe, lh)
            block = jnp.where(first, mine[...], other[...])
        else:
            mine, other = (lpe, lp) if n < 4 else (lp, lpe)
            block = jnp.where(first, mine[n % 2], other[n % 2])
        at = 128 * n
        compt[:, at : at + 128] = block[0:512]
        kpt[128:192, at : at + 128] = block[512:576]
        ktag[8 * n : 8 * n + 8] = block[576:592].astype(F32)[0:8]
    kpt[192:256] = jnp.zeros((64, NK), BF)
    kpt[0:128] = mm(ku[...].T, compt[...], NN).astype(BF)
    pairs = [(qp, qp_hbm), (do, do_hbm), (compt, compt_hbm), (kpt, kpt_hbm), (qtag, qtag_hbm), (ktag, ktag_hbm)]
    copies = copied(pairs, sems)
    v[...] = mm(vu[...].T, compt[...], NN).astype(BF).T
    kp[...] = kpt[...].T
    copies += copied([(kp, kp_hbm), (v, v_hbm)], late_sems)
    stats[...] = jnp.zeros_like(stats)
    statistics(1536, qp, do, qtag, kp, v, ktag, stats, 0)
    for copy in copies:
        copy.wait()


def forward_far(qz, kp, v, ktag, near, qp_hbm, do_hbm, qtag_hbm, stats, qp, do, qtag, own, sems):
    take_queries([qz[i] for i in range(4)], qp, do, qtag)
    copies = copied([(qp, qp_hbm), (do, do_hbm), (qtag, qtag_hbm)], sems)
    own[...] = jnp.zeros((8, 512), F32)
    statistics(512, qp, do, qtag, kp, v, ktag, own, 0)
    for p in range(3):
        stats[4 * p : 4 * p + 4] = near[0:4, 512 * p : 512 * p + 512]
    stats[12:16] = own[0:4]
    for copy in copies:
        copy.wait()


START = {0: 0, 1: 512, 3: 1024, 2: 1536}


def backward(*refs):
    there, (s0, s1, s2, s3), zpay, xpay, up = refs[:11], refs[11:15], refs[15:19], refs[19:23], refs[23]
    (dk, dv, low), here, sems = refs[24:27], refs[27:38], refs[38]
    kp, ktag, qp, qtag, v, do, kpt, qp2, qtag2, do2, compt = here
    copies = copied(list(zip(there, here)), sems)
    copies[1].wait()
    late = lateness()
    ktags = [ktag[8 * n : 8 * n + 1] for n in range(8)]
    stats = [s0, s1, s2, s3]
    for r in range(4):
        rows = []
        for d in range(4):
            at = START[(r - d) % 4] // 128
            rows.append([stats[d][at + n : at + n + 1] for n in range(3)])
        top = functools.reduce(jnp.maximum, [t[0] for t in rows])
        total = sum(t[1] * jnp.exp2(t[0] - top) for t in rows)
        weighted = sum(t[2] * jnp.exp2(t[0] - top) for t in rows)
        at = START[r]
        low[0:1, at : at + 512] = top + jnp.log2(total)
        low[1:2, at : at + 512] = weighted / total
    dk[...] = jnp.zeros_like(dk)
    dv[...] = jnp.zeros_like(dv)
    for n in (0, 2, 3, 4, 5, 6):
        copies[n].wait()
    for r in (0, 1, 3, 2):
        if r == 2:
            for copy in copies[7:10]:
                copy.wait()
        for i in range(2):
            to = START[r] + i * TQ
            if r == 2:
                q, g, qt = qp2[i * TQ : i * TQ + TQ], do2[i * TQ : i * TQ + TQ], qtag2[0:1, i * TQ : i * TQ + TQ]
            else:
                q, g, qt = qp[to : to + TQ], do[to : to + TQ], qtag[0:1, to : to + TQ]
            raw = mm(kp[...], q, NT)
            s = masked_scores(raw, [qt[:, 0:128], qt[:, 128:256]], ktags, late)
            p = jnp.exp2(s - low[0:1, to : to + TQ])
            dp = mm(v[...], g, NT)
            ds = (p * (dp - low[1:2, to : to + TQ])).astype(BF)
            dk[...] += mm(ds, q, NN)
            dv[...] += mm(p.astype(BF), g, NN)
            dq = (mm(kpt[...], ds, NN).T * SCALE).astype(BF)
            for b in range(2):
                m = 2 * i + b
                zpay[r][128 * m : 128 * m + 128] = dq[128 * b : 128 * b + 128, 0:128]
                zpay[r][512 + 64 * m : 576 + 64 * m] = dense_rope(dq[128 * b : 128 * b + 128, 128:192])
    dk16 = (dk[...] * SCALE).astype(BF)
    dv16 = dv[...].astype(BF)
    drope = dk16[:, 128:256].T
    for n in range(8):
        r, m = n // 2, n % 2
        xpay[r][128 * m : 128 * m + 128] = dk16[128 * n : 128 * n + 128, 0:128]
        xpay[r][256 + 128 * m : 384 + 128 * m] = dv16[128 * n : 128 * n + 128]
        xpay[r][512 + 64 * m : 576 + 64 * m] = drope[0:64, 128 * n : 128 * n + 128]
    copies[10].wait()
    both = mm(compt[...], jnp.concatenate([dk16[:, 0:128], dv16], axis=1), NN).astype(BF)
    for y in range(2):
        for z in range(4):
            at = 128 * z + 64 * y
            up[4 * y + z, 0:64] = both[at : at + 64, 0:128]
            up[4 * y + z, 64:128] = both[at : at + 64, 128:256]


def sum_queries(z0, z1, z2, z3, q0, q1, q2, q3):
    def total(rows):
        return sum(a[rows].astype(F32) for a in (z0, z1, z2, z3)).astype(BF)

    for r, back in enumerate((q0, q1, q2, q3)):
        back[0:128] = total(slice(128 * r, 128 * r + 128))
        back[128:192] = total(slice(512 + 64 * r, 576 + 64 * r))


def fold(x, x0, x1, x2, x3, ku, vu, pay, lat):
    acc = jnp.zeros((512, 256), F32)
    rope = jnp.zeros((128, 128), F32)
    for r, p in enumerate((x0, x1, x2, x3)):
        h = pl.multiple_of(lax.rem(x[0] + 4 - r, 4) * 128, 128)
        acc += mm(ku[:, pl.ds(h, 128)], p[0:256], NT)
        acc += mm(vu[:, pl.ds(h, 128)], p[256:512], NT)
        rope += p[512:640].astype(F32)
    lat[0:512] = acc[:, 0:128]
    lat[512:576] = rope[0:64]
    pay[0:512] = acc[:, 128:256].astype(BF)
    pay[512:576] = rope[64:128].astype(BF)


def spread(parts, every):
    mine = sum(parts[n].astype(F32) for n in range(8)).astype(BF)
    for n in range(32):
        every[n] = mine


def unpack_query_grad(x, q0, q1, q2, q3, out, heads):
    for r, ref in enumerate((q0, q1, q2, q3)):
        heads[(x[0] + r) & 3] = ref[...]
    for h in range(4):
        out[:, 192 * h : 192 * h + 128] = heads[h, 0:128]
        out[:, 192 * h + 128 : 192 * h + 192] = wide_rope(heads[h, 128:192])


def unpack_up(a, key, value):
    for y in range(2):
        for z in range(4):
            for x in range(4):
                part = a[place(y, z, x)].astype(F32)
                at = 128 * z + 64 * y
                key[at : at + 64, 128 * x : 128 * x + 128] = part[0:64]
                value[at : at + 64, 128 * x : 128 * x + 128] = part[64:128]


def shards(queries, latents, key_up, value_up, out_grad, positions):
    here = lax.axis_index("seq").astype(jnp.int32)
    x = here & 3
    part = ((QP, 128), BF)
    own, to1, to2, to3, lat = call(
        pack,
        [part, part, part, part, ((LP, 128), BF)],
        [(positions, HB), (x[None], SM), (queries, HB), (out_grad, HB), (latents.T, HB)],
        scratch=[
            pltpu.VMEM((ROWS, 768), BF), pltpu.VMEM((ROWS, 512), BF), pltpu.VMEM((4, QP, 128), BF),
            pltpu.SMEM((ROWS,), jnp.int32), pltpu.SemaphoreType.DMA((4,)),
        ],
    )
    core = lax.axis_index("head").astype(jnp.int32) & 1
    lat_y = along(lat, dy=1)
    q_1 = along(to1, dx=1)
    q_3 = along(to3, dx=-1)
    q_2 = along(to2, dx=2)
    pair = jnp.stack([lat, lat_y])
    q0 = jnp.stack([own, q_1, q_2, q_3])
    lp = by_core(pair, 1)
    lh = by_core(lax.dynamic_index_in_dim(pair, core, 0, keepdims=False), 2)
    qa = along(q0, dz=1)
    qb = along(q0, dz=-1)
    lpe = to_core(lp)
    lhe = to_core(lh)
    qz = along(q0, dz=2)
    ku = lax.dynamic_slice(key_up, (0, x * 128), (D_LAT, 128))
    vu = lax.dynamic_slice(value_up, (0, x * 128), (D_LAT, 128))

    flops = 2 * NQ * NK * 512
    near = [
        ((1536, 256), BF), ((1536, 128), BF), ((512, NK), BF), ((256, NK), BF), ((8, 1536), F32),
        ((NK, 256), BF), ((NK, 128), BF), ((64, 128), F32),
    ]
    qp, do, compt, kpt, qtag, kp, v, ktag, kp_here, v_here, ktag_here, stats = call(
        forward_near,
        [(*o, HB) for o in near] + near[5:8] + [((8, 1536), F32)],
        [(core[None], SM), q0, qa, qb, pair, lp, lpe, lh, lhe, ku, vu],
        scratch=[pltpu.VMEM(*o) for o in near[:5]] + [pltpu.SemaphoreType.DMA((6,)), pltpu.SemaphoreType.DMA((2,))],
        flops=flops * 3 // 4, grant=20,
    )
    far = [((512, 256), BF), ((512, 128), BF), ((8, 512), F32)]
    qp2, do2, qtag2, stats = call(
        forward_far,
        [(*o, HB) for o in far] + [((16, 512), F32)],
        [qz, kp_here, v_here, ktag_here, stats],
        scratch=[pltpu.VMEM(*o) for o in far] + [pltpu.VMEM((8, 512), F32), pltpu.SemaphoreType.DMA((3,))],
        flops=flops // 4, grant=12,
    )
    s3 = along(stats, dz=1)
    s1 = along(stats, dz=-1)
    s2 = along(stats, dz=2)

    there = [kp, ktag, qp, qtag, v, do, kpt, qp2, qtag2, do2, compt]
    pays = call(
        backward,
        [((768, 128), BF)] * 4 + [((640, 128), BF)] * 4 + [((8, 128, 128), BF)],
        [(a, HB) for a in there] + [stats, s1, s2, s3],
        scratch=[
            pltpu.VMEM((NK, 256), F32), pltpu.VMEM((NK, 128), F32), pltpu.VMEM((8, NQ), F32),
            *[pltpu.VMEM(a.shape, a.dtype) for a in there], pltpu.SemaphoreType.DMA((11,)),
        ],
        flops=3 * flops, grant=24,
    )
    zpay, xpay, up = pays[:4], pays[4:8], pays[8]
    x1 = along(xpay[1], dx=1)
    x3 = along(xpay[3], dx=3)
    x2 = along(xpay[2], dx=2)
    ups = lax.all_to_all(up, "seq", 0, 0, tiled=True, axis_index_groups=YZ_GROUPS)
    z1 = along(zpay[1], dz=1)
    z3 = along(zpay[3], dz=3)
    z2 = along(zpay[2], dz=2)
    pay, mine = call(
        fold, [((576, 128), BF), ((576, 128), F32)],
        [(x[None], SM), xpay[0], x1, x2, x3, key_up, value_up],
        flops=2 * 256 * 512 * 1024, grant=10,
    )
    got = along(pay, dy=1)
    (every,) = call(spread, [((32, 128, 128), BF)], [ups])
    whole = lax.all_to_all(every, "seq", 0, 0, tiled=True)
    b0, b1, b2, b3 = call(sum_queries, [((192, 128), BF)] * 4, [zpay[0], z1, z2, z3])
    c1 = along(b1, dx=-1)
    c3 = along(b3, dx=-3)
    c2 = along(b2, dx=-2)
    lat16 = lax.reduce_precision(mine + got.astype(F32), 8, 7).astype(BF)
    near16 = to_core(lat16)
    two = lax.reduce_precision(lat16.astype(F32) + near16.astype(F32), 8, 7).astype(BF)
    far16 = lax.ppermute(two, "head", [(0, 2), (1, 3), (2, 0), (3, 1)])
    latent_grad = (two.astype(F32) + far16.astype(F32)).T
    (query_grad,) = call(
        unpack_query_grad, [((ROWS, 768), BF)], [(x[None], SM), b0, c1, c2, c3],
        scratch=[pltpu.VMEM((4, 192, 128), BF)],
    )
    key_up_grad, value_up_grad = call(unpack_up, [((512, 512), F32), ((512, 512), F32)], [whole])
    return (query_grad, latent_grad, key_up_grad, value_up_grad)


def solution(mesh):
    in_specs = (
        P("seq", "head"),
        P("seq", None),
        P(None, "head"),
        P(None, "head"),
        P("seq", "head"),
        P("seq"),
    )
    out_specs = (P("seq", "head"), P("seq", None), P(None, "head"), P(None, "head"))
    return jax.shard_map(shards, mesh=mesh, in_specs=in_specs, out_specs=out_specs, check_vma=False)
```

```python
import functools
import math

import jax
import jax.numpy as jnp
from jax import lax
from jax.experimental import pallas as pl
from jax.experimental.pallas import tpu as pltpu
from jax.sharding import PartitionSpec as P


BF = jnp.bfloat16
F32 = jnp.float32
D_LAT = 512
D_ROPE = 64
D_NOPE = 128
ROWS = 128
SCALE = 1.0 / math.sqrt(D_NOPE + D_ROPE)
SCALE2 = SCALE * math.log2(math.e)
NEG = -1e30
QP = 336
LP = 592
NQ = 2048
NK = 1024
TQ = 256


def place(y, z, x):
    return (y % 2) * 16 + (z % 4) * 4 + x % 4


def along(value, dy=0, dz=0, dx=0):
    pairs = [
        (place(y, z, x), place(y + dy, z + dz, x + dx))
        for y in range(2)
        for z in range(4)
        for x in range(4)
    ]
    return lax.ppermute(value, "seq", pairs)


def by_core(value, dx):
    pairs = []
    for y in range(2):
        for z in range(4):
            for x in range(4):
                for h in range(4):
                    step = dx if h % 2 == 0 else -dx
                    pairs.append((place(y, z, x) * 4 + h, place(y, z, x + step) * 4 + h))
    return lax.ppermute(value, ("seq", "head"), pairs)


def to_core(value):
    return lax.ppermute(value, "head", [(0, 1), (1, 0), (2, 3), (3, 2)])


YZ_GROUPS = [[4 * k + i for k in range(8)] for i in range(4)]
VM, SM, HB = pltpu.VMEM, pltpu.SMEM, pltpu.HBM


def call(kernel, outs, args, scratch=(), flops=0, grant=6):
    args = [arg if isinstance(arg, tuple) else (arg, VM) for arg in args]
    args = [(pltpu.with_memory_space_constraint(a, HB) if m is HB else a, m) for a, m in args]
    return pl.pallas_call(
        kernel,
        out_shape=[HB(o[0], o[1]) if o[2:] == (HB,) else jax.ShapeDtypeStruct(o[0], o[1]) for o in outs],
        in_specs=[pl.BlockSpec(memory_space=space) for _, space in args],
        out_specs=[pl.BlockSpec(memory_space=o[2] if len(o) > 2 else VM) for o in outs],
        scratch_shapes=list(scratch),
        cost_estimate=pl.CostEstimate(flops=max(flops, 1), bytes_accessed=1 << 20, transcendentals=0),
        compiler_params=pltpu.CompilerParams(vmem_limit_bytes=grant << 20),
    )(*[array for array, _ in args])


def dense_rope(block):
    return jnp.concatenate([block[0:64], block[64:128]], axis=1)


def wide_rope(block):
    return jnp.concatenate([block[:, 0:64], block[:, 64:128]], axis=0)


def pack(pos_hbm, x, q_hbm, g_hbm, lat_hbm, own, to1, to2, to3, lat, q, g, heads, pos, sems):
    copies = [
        pltpu.make_async_copy(q_hbm, q, sems.at[0]),
        pltpu.make_async_copy(g_hbm, g, sems.at[1]),
        pltpu.make_async_copy(lat_hbm, lat.at[0:576], sems.at[2]),
        pltpu.make_async_copy(pos_hbm, pos, sems.at[3]),
    ]
    for copy in copies:
        copy.start()
    copies.pop().wait()
    tag = jnp.full((16, 128), (pos[0] >> 7).astype(F32), F32).astype(BF)
    lat[576:592] = tag
    for copy in copies:
        copy.wait()
    for h in range(4):
        heads[h, 0:128] = q[:, 192 * h : 192 * h + 128]
        heads[h, 128:256] = g[:, 128 * h : 128 * h + 128]
        heads[h, 256:320] = dense_rope(q[:, 192 * h + 128 : 192 * h + 192])
        heads[h, 320:336] = tag
    for r, out in enumerate((own, to1, to2, to3)):
        out[...] = heads[(x[0] + r) & 3]


def masked_scores(raw, qtags, ktags, late):
    rows = []
    for kb in range(NK // 128):
        cols = []
        for qb in range(TQ // 128):
            part = raw[128 * kb : 128 * kb + 128, 128 * qb : 128 * qb + 128]
            seen = late <= (qtags[qb] - ktags[kb]) * 128.0
            cols.append(jnp.where(seen, part * SCALE2, NEG))
        rows.append(jnp.concatenate(cols, axis=1))
    return jnp.concatenate(rows, axis=0)


def lateness():
    shape = (128, 128)
    return (lax.broadcasted_iota(jnp.int32, shape, 0) - lax.broadcasted_iota(jnp.int32, shape, 1)).astype(F32)


NT = (((1,), (1,)), ((), ()))
NN = (((1,), (0,)), ((), ()))


def mm(a, b, dims):
    return lax.dot_general(a, b, dims, preferred_element_type=F32)


def take_queries(blocks, qp, do, qtag):
    zeros = jnp.zeros((128, 64), BF)
    for n, block in enumerate(blocks):
        at = 128 * n
        qp[at : at + 128, 0:128] = block[0:128]
        qp[at : at + 128, 128:256] = jnp.concatenate([wide_rope(block[256:320]), zeros], axis=1)
        do[at : at + 128] = block[128:256]
        qtag[0:8, at : at + 128] = block[320:336].astype(F32)[0:8]


def statistics(rows, qp, do, qtag, kp, v, ktag, stats, first):
    late = lateness()
    ktags = [ktag[8 * n : 8 * n + 1] for n in range(8)]
    stats[...] = jnp.zeros_like(stats)

    def turn(i, carry):
        at = pl.multiple_of(i * TQ, TQ)
        to = pl.multiple_of(first + i * TQ, TQ)
        raw = mm(kp[...], qp[pl.ds(at, TQ)], NT)
        qt = qtag[0:1, pl.ds(at, TQ)]
        s = masked_scores(raw, [qt[:, 0:128], qt[:, 128:256]], ktags, late)
        top = jnp.max(s, axis=0, keepdims=True)
        p = jnp.exp2(s - top)
        dp = mm(v[...], do[pl.ds(at, TQ)], NT)
        stats[0:1, pl.ds(to, TQ)] = top
        stats[1:2, pl.ds(to, TQ)] = jnp.sum(p, axis=0, keepdims=True)
        stats[2:3, pl.ds(to, TQ)] = jnp.sum(p * dp, axis=0, keepdims=True)
        return carry

    lax.fori_loop(0, rows // TQ, turn, 0)


def copied(pairs, sems):
    copies = [pltpu.make_async_copy(src, dst, sems.at[n]) for n, (src, dst) in enumerate(pairs)]
    for copy in copies:
        copy.start()
    return copies


def forward_own(
    core, q0, q1, pair, lp, lpe, lh, lhe, ku, vu,
    qp_hbm, do_hbm, qtag_hbm, compt_hbm, kpt_hbm, kp_hbm, v_hbm, ktag_hbm, kp, v, ktag, stats,
    qp, do, qtag, compt, kpt, sems, late_sems,
):
    take_queries([ref[i] for ref in (q0, q1) for i in range(2)], qp, do, qtag)
    first = core[0] == 0
    for n in range(8):
        if n < 2:
            block = pair[n]
        elif n in (4, 5):
            mine, other = (lh, lhe) if n == 4 else (lhe, lh)
            block = jnp.where(first, mine[...], other[...])
        else:
            mine, other = (lpe, lp) if n < 4 else (lp, lpe)
            block = jnp.where(first, mine[n % 2], other[n % 2])
        at = 128 * n
        compt[:, at : at + 128] = block[0:512]
        kpt[128:192, at : at + 128] = block[512:576]
        ktag[8 * n : 8 * n + 8] = block[576:592].astype(F32)[0:8]
    kpt[192:256] = jnp.zeros((64, NK), BF)
    kpt[0:128] = mm(ku[...].T, compt[...], NN).astype(BF)
    pairs = [(qp, qp_hbm), (do, do_hbm), (qtag, qtag_hbm), (compt, compt_hbm), (kpt, kpt_hbm), (ktag, ktag_hbm)]
    copies = copied(pairs, sems)
    v[...] = mm(vu[...].T, compt[...], NN).astype(BF).T
    kp[...] = kpt[...].T
    copies += copied([(kp, kp_hbm), (v, v_hbm)], late_sems)
    statistics(512, qp, do, qtag, kp, v, ktag, stats, 0)
    for copy in copies:
        copy.wait()


def forward_near(a0, a1, b0, b1, kp, v, ktag, qp_hbm, do_hbm, qtag_hbm, stats, qp, do, qtag, sems):
    take_queries([ref[i] for ref in (b0, b1, a0, a1) for i in range(2)], qp, do, qtag)
    copies = copied([(qp, qp_hbm), (do, do_hbm), (qtag, qtag_hbm)], sems)
    statistics(1024, qp, do, qtag, kp, v, ktag, stats, 0)
    for copy in copies:
        copy.wait()


def forward_far(qc, qd, kp, v, ktag, own, near, qp_hbm, do_hbm, qtag_hbm, stats, qp, do, qtag, far, sems):
    take_queries([ref[i] for ref in (qc, qd) for i in range(2)], qp, do, qtag)
    copies = copied([(qp, qp_hbm), (do, do_hbm), (qtag, qtag_hbm)], sems)
    statistics(512, qp, do, qtag, kp, v, ktag, far, 0)
    stats[0:4] = own[0:4]
    stats[4:8] = near[0:4, 0:512]
    stats[8:12] = near[0:4, 512:1024]
    stats[12:16] = far[0:4]
    for copy in copies:
        copy.wait()


START = {0: 0, 1: 512, 3: 1024, 2: 1536}


def backward(*refs):
    there, stats, zpay, xpay, up = refs[:14], refs[14:18], refs[18:22], refs[22:26], refs[26]
    (dk, dv, low), here, sems = refs[27:30], refs[30:44], refs[44]
    kp, qp0, v, do0, ktag, qtag0, kpt, qp1, do1, qtag1, qp2, do2, qtag2, compt = here
    copies = copied(list(zip(there, here)), sems)
    late = lateness()
    for r in range(4):
        rows = []
        for d in range(4):
            at = START[(r - d) % 4] // 128
            rows.append([stats[d][at + n : at + n + 1] for n in range(3)])
        top = functools.reduce(jnp.maximum, [t[0] for t in rows])
        total = sum(t[1] * jnp.exp2(t[0] - top) for t in rows)
        weighted = sum(t[2] * jnp.exp2(t[0] - top) for t in rows)
        at = START[r]
        low[0:1, at : at + 512] = top + jnp.log2(total)
        low[1:2, at : at + 512] = weighted / total
    dk[...] = jnp.zeros_like(dk)
    dv[...] = jnp.zeros_like(dv)
    for copy in copies[:7]:
        copy.wait()
    ktags = [ktag[8 * n : 8 * n + 1] for n in range(8)]
    for r in (0, 1, 3, 2):
        if r == 1:
            for copy in copies[7:10]:
                copy.wait()
        if r == 2:
            for copy in copies[10:13]:
                copy.wait()
        qp, do, qtag = {0: (qp0, do0, qtag0), 2: (qp2, do2, qtag2)}.get(r, (qp1, do1, qtag1))
        for i in range(2):
            to = START[r] + i * TQ
            at = i * TQ + (512 if r == 3 else 0)
            q, g, qt = qp[at : at + TQ], do[at : at + TQ], qtag[0:1, at : at + TQ]
            raw = mm(kp[...], q, NT)
            s = masked_scores(raw, [qt[:, 0:128], qt[:, 128:256]], ktags, late)
            p = jnp.exp2(s - low[0:1, to : to + TQ])
            dp = mm(v[...], g, NT)
            ds = (p * (dp - low[1:2, to : to + TQ])).astype(BF)
            dk[...] += mm(ds, q, NN)
            dv[...] += mm(p.astype(BF), g, NN)
            dq = (mm(kpt[...], ds, NN).T * SCALE).astype(BF)
            for b in range(2):
                m = 2 * i + b
                zpay[r][128 * m : 128 * m + 128] = dq[128 * b : 128 * b + 128, 0:128]
                zpay[r][512 + 64 * m : 576 + 64 * m] = dense_rope(dq[128 * b : 128 * b + 128, 128:192])
    dk16 = (dk[...] * SCALE).astype(BF)
    dv16 = dv[...].astype(BF)
    drope = dk16[:, 128:256].T
    for n in range(8):
        r, m = n // 2, n % 2
        xpay[r][128 * m : 128 * m + 128] = dk16[128 * n : 128 * n + 128, 0:128]
        xpay[r][256 + 128 * m : 384 + 128 * m] = dv16[128 * n : 128 * n + 128]
        xpay[r][512 + 64 * m : 576 + 64 * m] = drope[0:64, 128 * n : 128 * n + 128]
    copies[13].wait()
    both = mm(compt[...], jnp.concatenate([dk16[:, 0:128], dv16], axis=1), NN).astype(BF)
    for y in range(2):
        for z in range(4):
            at = 128 * z + 64 * y
            up[4 * y + z, 0:64] = both[at : at + 64, 0:128]
            up[4 * y + z, 64:128] = both[at : at + 64, 128:256]


def sum_queries(z0, z1, z2, z3, q0, q1, q2, q3):
    def total(rows):
        return sum(a[rows].astype(F32) for a in (z0, z1, z2, z3)).astype(BF)

    for r, back in enumerate((q0, q1, q2, q3)):
        back[0:128] = total(slice(128 * r, 128 * r + 128))
        back[128:192] = total(slice(512 + 64 * r, 576 + 64 * r))


def fold(x, x0, x1, x2, x3, ku, vu, pay, lat):
    acc = jnp.zeros((512, 256), F32)
    rope = jnp.zeros((128, 128), F32)
    for r, p in enumerate((x0, x1, x2, x3)):
        h = pl.multiple_of(lax.rem(x[0] + 4 - r, 4) * 128, 128)
        acc += mm(ku[:, pl.ds(h, 128)], p[0:256], NT)
        acc += mm(vu[:, pl.ds(h, 128)], p[256:512], NT)
        rope += p[512:640].astype(F32)
    lat[0:512] = acc[:, 0:128]
    lat[512:576] = rope[0:64]
    pay[0:512] = acc[:, 128:256].astype(BF)
    pay[512:576] = rope[64:128].astype(BF)


def spread(parts, every):
    mine = sum(parts[n].astype(F32) for n in range(8)).astype(BF)
    for n in range(32):
        every[n] = mine


def unpack_query_grad(x, q0, q1, q2, q3, out, heads):
    for r, ref in enumerate((q0, q1, q2, q3)):
        heads[(x[0] + r) & 3] = ref[...]
    for h in range(4):
        out[:, 192 * h : 192 * h + 128] = heads[h, 0:128]
        out[:, 192 * h + 128 : 192 * h + 192] = wide_rope(heads[h, 128:192])


def unpack_up(a, key, value):
    for y in range(2):
        for z in range(4):
            for x in range(4):
                part = a[place(y, z, x)].astype(F32)
                at = 128 * z + 64 * y
                key[at : at + 64, 128 * x : 128 * x + 128] = part[0:64]
                value[at : at + 64, 128 * x : 128 * x + 128] = part[64:128]


def shards(queries, latents, key_up, value_up, out_grad, positions):
    here = lax.axis_index("seq").astype(jnp.int32)
    x = here & 3
    part = ((QP, 128), BF)
    own, to1, to2, to3, lat = call(
        pack,
        [part, part, part, part, ((LP, 128), BF)],
        [(positions, HB), (x[None], SM), (queries, HB), (out_grad, HB), (latents.T, HB)],
        scratch=[
            pltpu.VMEM((ROWS, 768), BF), pltpu.VMEM((ROWS, 512), BF), pltpu.VMEM((4, QP, 128), BF),
            pltpu.SMEM((ROWS,), jnp.int32), pltpu.SemaphoreType.DMA((4,)),
        ],
    )
    core = lax.axis_index("head").astype(jnp.int32) & 1
    lat_y = along(lat, dy=1)
    q_1 = along(to1, dx=1)
    q_3 = along(to3, dx=-1)
    q_2 = along(to2, dx=2)
    pair = jnp.stack([lat, lat_y])
    q0 = jnp.stack([own, q_1])
    q1 = jnp.stack([q_2, q_3])
    lp = by_core(pair, 1)
    lh = by_core(lax.dynamic_index_in_dim(pair, core, 0, keepdims=False), 2)
    qa0 = along(q0, dz=1)
    qb0 = along(q0, dz=-1)
    qa1 = along(q1, dz=1)
    qb1 = along(q1, dz=-1)
    qc = along(qa0, dz=1)
    qd = along(qb1, dz=-1)
    lpe = to_core(lp)
    lhe = to_core(lh)
    ku = lax.dynamic_slice(key_up, (0, x * 128), (D_LAT, 128))
    vu = lax.dynamic_slice(value_up, (0, x * 128), (D_LAT, 128))

    flops = 2 * NQ * NK * 512

    def rows(n):
        return [((n, 256), BF), ((n, 128), BF), ((8, n), F32)]

    def at_hbm(shapes):
        return [(*o, HB) for o in shapes]

    def at_vmem(shapes):
        return [pltpu.VMEM(*o) for o in shapes]

    wide = [((512, NK), BF), ((256, NK), BF)]
    keyed = [((NK, 256), BF), ((NK, 128), BF), ((64, 128), F32)]
    qp0, do0, qtag0, compt, kpt, kp, v, ktag, *here, own_stats = call(
        forward_own,
        at_hbm(rows(512) + wide + keyed) + keyed + [((8, 512), F32)],
        [(core[None], SM), q0, q1, pair, lp, lpe, lh, lhe, ku, vu],
        scratch=at_vmem(rows(512) + wide) + [pltpu.SemaphoreType.DMA((6,)), pltpu.SemaphoreType.DMA((2,))],
        flops=flops // 4, grant=20,
    )
    qp1, do1, qtag1, near_stats = call(
        forward_near,
        at_hbm(rows(1024)) + [((8, 1024), F32)],
        [qa0, qa1, qb0, qb1, *here],
        scratch=at_vmem(rows(1024)) + [pltpu.SemaphoreType.DMA((3,))],
        flops=flops // 2, grant=14,
    )
    qp2, do2, qtag2, stats = call(
        forward_far,
        at_hbm(rows(512)) + [((16, 512), F32)],
        [qc, qd, *here, own_stats, near_stats],
        scratch=at_vmem(rows(512)) + [pltpu.VMEM((8, 512), F32), pltpu.SemaphoreType.DMA((3,))],
        flops=flops // 4, grant=12,
    )
    s1 = along(stats, dz=-1)
    s3 = along(stats, dz=1)
    s2 = along(stats, dz=2)

    there = [kp, qp0, v, do0, ktag, qtag0, kpt, qp1, do1, qtag1, qp2, do2, qtag2, compt]
    pays = call(
        backward,
        [((768, 128), BF)] * 4 + [((640, 128), BF)] * 4 + [((8, 128, 128), BF)],
        [(a, HB) for a in there] + [stats, s1, s2, s3],
        scratch=[
            pltpu.VMEM((NK, 256), F32), pltpu.VMEM((NK, 128), F32), pltpu.VMEM((8, NQ), F32),
            *[pltpu.VMEM(a.shape, a.dtype) for a in there], pltpu.SemaphoreType.DMA((14,)),
        ],
        flops=3 * flops, grant=24,
    )
    zpay, xpay, up = pays[:4], pays[4:8], pays[8]
    x1 = along(xpay[1], dx=1)
    x3 = along(xpay[3], dx=3)
    x2 = along(xpay[2], dx=2)
    ups = lax.all_to_all(up, "seq", 0, 0, tiled=True, axis_index_groups=YZ_GROUPS)
    z1 = along(zpay[1], dz=1)
    z3 = along(zpay[3], dz=3)
    z2 = along(zpay[2], dz=2)
    pay, mine = call(
        fold, [((576, 128), BF), ((576, 128), F32)],
        [(x[None], SM), xpay[0], x1, x2, x3, key_up, value_up],
        flops=2 * 256 * 512 * 1024, grant=10,
    )
    got = along(pay, dy=1)
    (every,) = call(spread, [((32, 128, 128), BF)], [ups])
    whole = lax.all_to_all(every, "seq", 0, 0, tiled=True)
    b0, b1, b2, b3 = call(sum_queries, [((192, 128), BF)] * 4, [zpay[0], z1, z2, z3])
    c1 = along(b1, dx=-1)
    c3 = along(b3, dx=-3)
    c2 = along(b2, dx=-2)
    lat16 = lax.reduce_precision(mine + got.astype(F32), 8, 7).astype(BF)
    near16 = to_core(lat16)
    two = lax.reduce_precision(lat16.astype(F32) + near16.astype(F32), 8, 7).astype(BF)
    far16 = lax.ppermute(two, "head", [(0, 2), (1, 3), (2, 0), (3, 1)])
    latent_grad = (two.astype(F32) + far16.astype(F32)).T
    (query_grad,) = call(
        unpack_query_grad, [((ROWS, 768), BF)], [(x[None], SM), b0, c1, c2, c3],
        scratch=[pltpu.VMEM((4, 192, 128), BF)],
    )
    key_up_grad, value_up_grad = call(unpack_up, [((512, 512), F32), ((512, 512), F32)], [whole])
    return (query_grad, latent_grad, key_up_grad, value_up_grad)


def solution(mesh):
    in_specs = (
        P("seq", "head"),
        P("seq", None),
        P(None, "head"),
        P(None, "head"),
        P("seq", "head"),
        P("seq"),
    )
    out_specs = (P("seq", "head"), P("seq", None), P(None, "head"), P(None, "head"))
    return jax.shard_map(shards, mesh=mesh, in_specs=in_specs, out_specs=out_specs, check_vma=False)
```

```python
import functools
import math

import jax
import jax.numpy as jnp
from jax import lax
from jax.experimental import pallas as pl
from jax.experimental.pallas import tpu as pltpu
from jax.sharding import PartitionSpec as P


BF = jnp.bfloat16
F32 = jnp.float32
D_LAT = 512
D_ROPE = 64
D_NOPE = 128
ROWS = 128
SCALE = 1.0 / math.sqrt(D_NOPE + D_ROPE)
SCALE2 = SCALE * math.log2(math.e)
NEG = -1e30
QP = 336
LP = 592
NQ = 2048
NK = 1024
TQ = 256


def place(y, z, x):
    return (y % 2) * 16 + (z % 4) * 4 + x % 4


def along(value, dy=0, dz=0, dx=0):
    pairs = [
        (place(y, z, x), place(y + dy, z + dz, x + dx))
        for y in range(2)
        for z in range(4)
        for x in range(4)
    ]
    return lax.ppermute(value, "seq", pairs)


def by_core(value, dx):
    pairs = []
    for y in range(2):
        for z in range(4):
            for x in range(4):
                for h in range(4):
                    step = dx if h % 2 == 0 else -dx
                    pairs.append((place(y, z, x) * 4 + h, place(y, z, x + step) * 4 + h))
    return lax.ppermute(value, ("seq", "head"), pairs)


def to_core(value):
    return lax.ppermute(value, "head", [(0, 1), (1, 0), (2, 3), (3, 2)])


YZ_GROUPS = [[4 * k + i for k in range(8)] for i in range(4)]
VM, SM, HB = pltpu.VMEM, pltpu.SMEM, pltpu.HBM


def call(kernel, outs, args, scratch=(), flops=0, grant=6):
    args = [arg if isinstance(arg, tuple) else (arg, VM) for arg in args]
    args = [(pltpu.with_memory_space_constraint(a, HB) if m is HB else a, m) for a, m in args]
    return pl.pallas_call(
        kernel,
        out_shape=[HB(o[0], o[1]) if o[2:] == (HB,) else jax.ShapeDtypeStruct(o[0], o[1]) for o in outs],
        in_specs=[pl.BlockSpec(memory_space=space) for _, space in args],
        out_specs=[pl.BlockSpec(memory_space=o[2] if len(o) > 2 else VM) for o in outs],
        scratch_shapes=list(scratch),
        cost_estimate=pl.CostEstimate(flops=max(flops, 1), bytes_accessed=1 << 20, transcendentals=0),
        compiler_params=pltpu.CompilerParams(vmem_limit_bytes=grant << 20),
    )(*[array for array, _ in args])


def dense_rope(block):
    return jnp.concatenate([block[0:64], block[64:128]], axis=1)


def wide_rope(block):
    return jnp.concatenate([block[:, 0:64], block[:, 64:128]], axis=0)


def pack(pos_hbm, x, q_hbm, g_hbm, lat_hbm, own, to1, to2, to3, lat, q, g, heads, pos, sems):
    copies = [
        pltpu.make_async_copy(q_hbm, q, sems.at[0]),
        pltpu.make_async_copy(g_hbm, g, sems.at[1]),
        pltpu.make_async_copy(lat_hbm, lat.at[0:576], sems.at[2]),
        pltpu.make_async_copy(pos_hbm, pos, sems.at[3]),
    ]
    for copy in copies:
        copy.start()
    copies.pop().wait()
    tag = jnp.full((16, 128), (pos[0] >> 7).astype(F32), F32).astype(BF)
    lat[576:592] = tag
    for copy in copies:
        copy.wait()
    for h in range(4):
        heads[h, 0:128] = q[:, 192 * h : 192 * h + 128]
        heads[h, 128:256] = g[:, 128 * h : 128 * h + 128]
        heads[h, 256:320] = dense_rope(q[:, 192 * h + 128 : 192 * h + 192])
        heads[h, 320:336] = tag
    for r, out in enumerate((own, to1, to2, to3)):
        out[...] = heads[(x[0] + r) & 3]


def masked_scores(raw, qtags, ktags, late):
    rows = []
    for kb in range(NK // 128):
        cols = []
        for qb in range(TQ // 128):
            part = raw[128 * kb : 128 * kb + 128, 128 * qb : 128 * qb + 128]
            seen = late <= (qtags[qb] - ktags[kb]) * 128.0
            cols.append(jnp.where(seen, part * SCALE2, NEG))
        rows.append(jnp.concatenate(cols, axis=1))
    return jnp.concatenate(rows, axis=0)


def lateness():
    shape = (128, 128)
    return (lax.broadcasted_iota(jnp.int32, shape, 0) - lax.broadcasted_iota(jnp.int32, shape, 1)).astype(F32)


NT = (((1,), (1,)), ((), ()))
NN = (((1,), (0,)), ((), ()))


def mm(a, b, dims):
    return lax.dot_general(a, b, dims, preferred_element_type=F32)


def take_queries(blocks, qp, do, qtag):
    zeros = jnp.zeros((128, 64), BF)
    for n, block in enumerate(blocks):
        at = 128 * n
        qp[at : at + 128, 0:128] = block[0:128]
        qp[at : at + 128, 128:256] = jnp.concatenate([wide_rope(block[256:320]), zeros], axis=1)
        do[at : at + 128] = block[128:256]
        qtag[0:8, at : at + 128] = block[320:336].astype(F32)[0:8]


def statistics(rows, qp, do, qtag, kp, v, ktag, stats, first):
    late = lateness()
    ktags = [ktag[8 * n : 8 * n + 1] for n in range(8)]
    stats[...] = jnp.zeros_like(stats)

    def turn(i, carry):
        at = pl.multiple_of(i * TQ, TQ)
        to = pl.multiple_of(first + i * TQ, TQ)
        raw = mm(kp[...], qp[pl.ds(at, TQ)], NT)
        qt = qtag[0:1, pl.ds(at, TQ)]
        s = masked_scores(raw, [qt[:, 0:128], qt[:, 128:256]], ktags, late)
        top = jnp.max(s, axis=0, keepdims=True)
        p = jnp.exp2(s - top)
        dp = mm(v[...], do[pl.ds(at, TQ)], NT)
        stats[0:1, pl.ds(to, TQ)] = top
        stats[1:2, pl.ds(to, TQ)] = jnp.sum(p, axis=0, keepdims=True)
        stats[2:3, pl.ds(to, TQ)] = jnp.sum(p * dp, axis=0, keepdims=True)
        return carry

    lax.fori_loop(0, rows // TQ, turn, 0)


def copied(pairs, sems, first=0):
    copies = [pltpu.make_async_copy(src, dst, sems.at[first + n]) for n, (src, dst) in enumerate(pairs)]
    for copy in copies:
        copy.start()
    return copies


def forward_own(
    core, q0, q1, pair, lp, lpe, lh, lhe, ku, vu,
    qp_hbm, do_hbm, qtag_hbm, compt_hbm, kpt_hbm, kp_hbm, v_hbm, ktag_hbm, kp, v, ktag, stats,
    qp, do, qtag, compt, kpt, sems, late_sems,
):
    take_queries([ref[i] for ref in (q0, q1) for i in range(2)], qp, do, qtag)
    first = core[0] == 0
    for n in range(8):
        if n < 2:
            block = pair[n]
        elif n in (4, 5):
            mine, other = (lh, lhe) if n == 4 else (lhe, lh)
            block = jnp.where(first, mine[...], other[...])
        else:
            mine, other = (lpe, lp) if n < 4 else (lp, lpe)
            block = jnp.where(first, mine[n % 2], other[n % 2])
        at = 128 * n
        compt[:, at : at + 128] = block[0:512]
        kpt[128:192, at : at + 128] = block[512:576]
        ktag[8 * n : 8 * n + 8] = block[576:592].astype(F32)[0:8]
    kpt[192:256] = jnp.zeros((64, NK), BF)
    kpt[0:128] = mm(ku[...].T, compt[...], NN).astype(BF)
    pairs = [(qp, qp_hbm), (do, do_hbm), (qtag, qtag_hbm), (compt, compt_hbm), (kpt, kpt_hbm), (ktag, ktag_hbm)]
    copies = copied(pairs, sems)
    v[...] = mm(vu[...].T, compt[...], NN).astype(BF).T
    kp[...] = kpt[...].T
    copies += copied([(kp, kp_hbm), (v, v_hbm)], late_sems)
    statistics(512, qp, do, qtag, kp, v, ktag, stats, 0)
    for copy in copies:
        copy.wait()


def forward_near(a0, a1, b0, b1, kp, v, ktag, qp_hbm, do_hbm, qtag_hbm, stats, qp, do, qtag, sems):
    take_queries([ref[i] for ref in (b0, b1, a0, a1) for i in range(2)], qp, do, qtag)
    copies = copied([(qp, qp_hbm), (do, do_hbm), (qtag, qtag_hbm)], sems)
    statistics(1024, qp, do, qtag, kp, v, ktag, stats, 0)
    for copy in copies:
        copy.wait()


def forward_far(qc, qd, kp, v, ktag, own, near, qp_hbm, do_hbm, qtag_hbm, stats, qp, do, qtag, far, sems):
    take_queries([ref[i] for ref in (qc, qd) for i in range(2)], qp, do, qtag)
    copies = copied([(qp, qp_hbm), (do, do_hbm), (qtag, qtag_hbm)], sems)
    statistics(512, qp, do, qtag, kp, v, ktag, far, 0)
    stats[0:4] = own[0:4]
    stats[4:8] = near[0:4, 0:512]
    stats[8:12] = near[0:4, 512:1024]
    stats[12:16] = far[0:4]
    for copy in copies:
        copy.wait()


START = {0: 0, 1: 512, 3: 1024, 2: 1536}


def backward(*refs):
    there, stats, zpay, xpay, up = refs[:14], refs[14:18], refs[18:22], refs[22:26], refs[26]
    (dk, dv, low), here, sems = refs[27:30], refs[30:44], refs[44]
    kp, qp0, v, do0, ktag, qtag0, kpt, qp1, do1, qtag1, qp2, do2, qtag2, compt = here
    pairs = list(zip(there, here))
    copies = copied(pairs[:6], sems)
    late = lateness()
    for r in range(4):
        rows = []
        for d in range(4):
            at = START[(r - d) % 4] // 128
            rows.append([stats[d][at + n : at + n + 1] for n in range(3)])
        top = functools.reduce(jnp.maximum, [t[0] for t in rows])
        total = sum(t[1] * jnp.exp2(t[0] - top) for t in rows)
        weighted = sum(t[2] * jnp.exp2(t[0] - top) for t in rows)
        at = START[r]
        low[0:1, at : at + 512] = top + jnp.log2(total)
        low[1:2, at : at + 512] = weighted / total
    dk[...] = jnp.zeros_like(dk)
    dv[...] = jnp.zeros_like(dv)
    for copy in copies:
        copy.wait()
    copies += copied(pairs[6:], sems, 6)
    ktags = [ktag[8 * n : 8 * n + 1] for n in range(8)]
    for r in (0, 1, 3, 2):
        if r == 1:
            for copy in copies[7:10]:
                copy.wait()
        if r == 2:
            for copy in copies[10:13]:
                copy.wait()
        qp, do, qtag = {0: (qp0, do0, qtag0), 2: (qp2, do2, qtag2)}.get(r, (qp1, do1, qtag1))
        for i in range(2):
            to = START[r] + i * TQ
            at = i * TQ + (512 if r == 3 else 0)
            q, g, qt = qp[at : at + TQ], do[at : at + TQ], qtag[0:1, at : at + TQ]
            raw = mm(kp[...], q, NT)
            s = masked_scores(raw, [qt[:, 0:128], qt[:, 128:256]], ktags, late)
            p = jnp.exp2(s - low[0:1, to : to + TQ])
            dp = mm(v[...], g, NT)
            ds = (p * (dp - low[1:2, to : to + TQ])).astype(BF)
            dk[...] += mm(ds, q, NN)
            dv[...] += mm(p.astype(BF), g, NN)
            if to == 0:
                copies[6].wait()
            dq = (mm(kpt[...], ds, NN).T * SCALE).astype(BF)
            for b in range(2):
                m = 2 * i + b
                zpay[r][128 * m : 128 * m + 128] = dq[128 * b : 128 * b + 128, 0:128]
                zpay[r][512 + 64 * m : 576 + 64 * m] = dense_rope(dq[128 * b : 128 * b + 128, 128:192])
    dk16 = (dk[...] * SCALE).astype(BF)
    dv16 = dv[...].astype(BF)
    drope = dk16[:, 128:256].T
    for n in range(8):
        r, m = n // 2, n % 2
        xpay[r][128 * m : 128 * m + 128] = dk16[128 * n : 128 * n + 128, 0:128]
        xpay[r][256 + 128 * m : 384 + 128 * m] = dv16[128 * n : 128 * n + 128]
        xpay[r][512 + 64 * m : 576 + 64 * m] = drope[0:64, 128 * n : 128 * n + 128]
    copies[13].wait()
    both = mm(compt[...], jnp.concatenate([dk16[:, 0:128], dv16], axis=1), NN).astype(BF)
    for y in range(2):
        for z in range(4):
            at = 128 * z + 64 * y
            up[4 * y + z, 0:64] = both[at : at + 64, 0:128]
            up[4 * y + z, 64:128] = both[at : at + 64, 128:256]


def sum_queries(z0, z1, z2, z3, q0, q1, q2, q3):
    def total(rows):
        return sum(a[rows].astype(F32) for a in (z0, z1, z2, z3)).astype(BF)

    for r, back in enumerate((q0, q1, q2, q3)):
        back[0:128] = total(slice(128 * r, 128 * r + 128))
        back[128:192] = total(slice(512 + 64 * r, 576 + 64 * r))


def fold(x, x0, x1, x2, x3, ku, vu, pay, lat):
    acc = jnp.zeros((512, 256), F32)
    rope = jnp.zeros((128, 128), F32)
    for r, p in enumerate((x0, x1, x2, x3)):
        h = pl.multiple_of(lax.rem(x[0] + 4 - r, 4) * 128, 128)
        acc += mm(ku[:, pl.ds(h, 128)], p[0:256], NT)
        acc += mm(vu[:, pl.ds(h, 128)], p[256:512], NT)
        rope += p[512:640].astype(F32)
    lat[0:512] = acc[:, 0:128]
    lat[512:576] = rope[0:64]
    pay[0:512] = acc[:, 128:256].astype(BF)
    pay[512:576] = rope[64:128].astype(BF)


def spread(parts, every):
    mine = sum(parts[n].astype(F32) for n in range(8)).astype(BF)
    for n in range(32):
        every[n] = mine


def unpack_query_grad(x, q0, q1, q2, q3, out, heads):
    for r, ref in enumerate((q0, q1, q2, q3)):
        heads[(x[0] + r) & 3] = ref[...]
    for h in range(4):
        out[:, 192 * h : 192 * h + 128] = heads[h, 0:128]
        out[:, 192 * h + 128 : 192 * h + 192] = wide_rope(heads[h, 128:192])


def unpack_up(a, key, value):
    for y in range(2):
        for z in range(4):
            for x in range(4):
                part = a[place(y, z, x)].astype(F32)
                at = 128 * z + 64 * y
                key[at : at + 64, 128 * x : 128 * x + 128] = part[0:64]
                value[at : at + 64, 128 * x : 128 * x + 128] = part[64:128]


def shards(queries, latents, key_up, value_up, out_grad, positions):
    here = lax.axis_index("seq").astype(jnp.int32)
    x = here & 3
    part = ((QP, 128), BF)
    own, to1, to2, to3, lat = call(
        pack,
        [part, part, part, part, ((LP, 128), BF)],
        [(positions, HB), (x[None], SM), (queries, HB), (out_grad, HB), (latents.T, HB)],
        scratch=[
            pltpu.VMEM((ROWS, 768), BF), pltpu.VMEM((ROWS, 512), BF), pltpu.VMEM((4, QP, 128), BF),
            pltpu.SMEM((ROWS,), jnp.int32), pltpu.SemaphoreType.DMA((4,)),
        ],
    )
    core = lax.axis_index("head").astype(jnp.int32) & 1
    lat_y = along(lat, dy=1)
    q_1 = along(to1, dx=1)
    q_3 = along(to3, dx=-1)
    q_2 = along(to2, dx=2)
    pair = jnp.stack([lat, lat_y])
    q0 = jnp.stack([own, q_1])
    q1 = jnp.stack([q_2, q_3])
    lp = by_core(pair, 1)
    lh = by_core(lax.dynamic_index_in_dim(pair, core, 0, keepdims=False), 2)
    qa0 = along(q0, dz=1)
    qb0 = along(q0, dz=-1)
    qa1 = along(q1, dz=1)
    qb1 = along(q1, dz=-1)
    qc = along(qa0, dz=1)
    qd = along(qb1, dz=-1)
    lpe = to_core(lp)
    lhe = to_core(lh)
    ku = lax.dynamic_slice(key_up, (0, x * 128), (D_LAT, 128))
    vu = lax.dynamic_slice(value_up, (0, x * 128), (D_LAT, 128))

    flops = 2 * NQ * NK * 512

    def rows(n):
        return [((n, 256), BF), ((n, 128), BF), ((8, n), F32)]

    def at_hbm(shapes):
        return [(*o, HB) for o in shapes]

    def at_vmem(shapes):
        return [pltpu.VMEM(*o) for o in shapes]

    wide = [((512, NK), BF), ((256, NK), BF)]
    keyed = [((NK, 256), BF), ((NK, 128), BF), ((64, 128), F32)]
    qp0, do0, qtag0, compt, kpt, kp, v, ktag, *here, own_stats = call(
        forward_own,
        at_hbm(rows(512) + wide + keyed) + keyed + [((8, 512), F32)],
        [(core[None], SM), q0, q1, pair, lp, lpe, lh, lhe, ku, vu],
        scratch=at_vmem(rows(512) + wide) + [pltpu.SemaphoreType.DMA((6,)), pltpu.SemaphoreType.DMA((2,))],
        flops=flops // 4, grant=20,
    )
    qp1, do1, qtag1, near_stats = call(
        forward_near,
        at_hbm(rows(1024)) + [((8, 1024), F32)],
        [qa0, qa1, qb0, qb1, *here],
        scratch=at_vmem(rows(1024)) + [pltpu.SemaphoreType.DMA((3,))],
        flops=flops // 2, grant=14,
    )
    qp2, do2, qtag2, stats = call(
        forward_far,
        at_hbm(rows(512)) + [((16, 512), F32)],
        [qc, qd, *here, own_stats, near_stats],
        scratch=at_vmem(rows(512)) + [pltpu.VMEM((8, 512), F32), pltpu.SemaphoreType.DMA((3,))],
        flops=flops // 4, grant=12,
    )
    s1 = along(stats, dz=-1)
    s3 = along(stats, dz=1)
    s2 = along(stats, dz=2)

    there = [kp, qp0, v, do0, ktag, qtag0, kpt, qp1, do1, qtag1, qp2, do2, qtag2, compt]
    pays = call(
        backward,
        [((768, 128), BF)] * 4 + [((640, 128), BF)] * 4 + [((8, 128, 128), BF)],
        [(a, HB) for a in there] + [stats, s1, s2, s3],
        scratch=[
            pltpu.VMEM((NK, 256), F32), pltpu.VMEM((NK, 128), F32), pltpu.VMEM((8, NQ), F32),
            *[pltpu.VMEM(a.shape, a.dtype) for a in there], pltpu.SemaphoreType.DMA((14,)),
        ],
        flops=3 * flops, grant=24,
    )
    zpay, xpay, up = pays[:4], pays[4:8], pays[8]
    x1 = along(xpay[1], dx=1)
    x3 = along(xpay[3], dx=3)
    x2 = along(xpay[2], dx=2)
    ups = lax.all_to_all(up, "seq", 0, 0, tiled=True, axis_index_groups=YZ_GROUPS)
    z1 = along(zpay[1], dz=1)
    z3 = along(zpay[3], dz=3)
    z2 = along(zpay[2], dz=2)
    pay, mine = call(
        fold, [((576, 128), BF), ((576, 128), F32)],
        [(x[None], SM), xpay[0], x1, x2, x3, key_up, value_up],
        flops=2 * 256 * 512 * 1024, grant=10,
    )
    got = along(pay, dy=1)
    (every,) = call(spread, [((32, 128, 128), BF)], [ups])
    whole = lax.all_to_all(every, "seq", 0, 0, tiled=True)
    b0, b1, b2, b3 = call(sum_queries, [((192, 128), BF)] * 4, [zpay[0], z1, z2, z3])
    c1 = along(b1, dx=-1)
    c3 = along(b3, dx=-3)
    c2 = along(b2, dx=-2)
    lat16 = lax.reduce_precision(mine + got.astype(F32), 8, 7).astype(BF)
    near16 = to_core(lat16)
    two = lax.reduce_precision(lat16.astype(F32) + near16.astype(F32), 8, 7).astype(BF)
    far16 = lax.ppermute(two, "head", [(0, 2), (1, 3), (2, 0), (3, 1)])
    latent_grad = (two.astype(F32) + far16.astype(F32)).T
    (query_grad,) = call(
        unpack_query_grad, [((ROWS, 768), BF)], [(x[None], SM), b0, c1, c2, c3],
        scratch=[pltpu.VMEM((4, 192, 128), BF)],
    )
    key_up_grad, value_up_grad = call(unpack_up, [((512, 512), F32), ((512, 512), F32)], [whole])
    return (query_grad, latent_grad, key_up_grad, value_up_grad)


def solution(mesh):
    in_specs = (
        P("seq", "head"),
        P("seq", None),
        P(None, "head"),
        P(None, "head"),
        P("seq", "head"),
        P("seq"),
    )
    out_specs = (P("seq", "head"), P("seq", None), P(None, "head"), P(None, "head"))
    return jax.shard_map(shards, mesh=mesh, in_specs=in_specs, out_specs=out_specs, check_vma=False)
```

```python
import functools
import math

import jax
import jax.numpy as jnp
from jax import lax
from jax.experimental import pallas as pl
from jax.experimental.pallas import tpu as pltpu
from jax.sharding import PartitionSpec as P


BF = jnp.bfloat16
F32 = jnp.float32
D_ROPE = 64
D_NOPE = 128
ROWS = 128
SCALE = 1.0 / math.sqrt(D_NOPE + D_ROPE)
SCALE2 = SCALE * math.log2(math.e)
NEG = -1e30
QP = 336
LP = 592
NQ = 2048
NK = 1024
TQ = 256


def place(y, z, x):
    return (y % 2) * 16 + (z % 4) * 4 + x % 4


def along(value, dy=0, dz=0, dx=0):
    pairs = [
        (place(y, z, x), place(y + dy, z + dz, x + dx))
        for y in range(2)
        for z in range(4)
        for x in range(4)
    ]
    return lax.ppermute(value, "seq", pairs)


def by_core(value, dx):
    pairs = []
    for y in range(2):
        for z in range(4):
            for x in range(4):
                for h in range(4):
                    step = dx if h % 2 == 0 else -dx
                    pairs.append((place(y, z, x) * 4 + h, place(y, z, x + step) * 4 + h))
    return lax.ppermute(value, ("seq", "head"), pairs)


def to_core(value):
    return lax.ppermute(value, "head", [(0, 1), (1, 0), (2, 3), (3, 2)])


YZ_GROUPS = [[4 * k + i for k in range(8)] for i in range(4)]
VM, SM, HB = pltpu.VMEM, pltpu.SMEM, pltpu.HBM


def call(kernel, outs, args, scratch=(), flops=0, grant=6):
    args = [arg if isinstance(arg, tuple) else (arg, VM) for arg in args]
    args = [(pltpu.with_memory_space_constraint(a, HB) if m is HB else a, m) for a, m in args]
    return pl.pallas_call(
        kernel,
        out_shape=[HB(o[0], o[1]) if o[2:] == (HB,) else jax.ShapeDtypeStruct(o[0], o[1]) for o in outs],
        in_specs=[pl.BlockSpec(memory_space=space) for _, space in args],
        out_specs=[pl.BlockSpec(memory_space=o[2] if len(o) > 2 else VM) for o in outs],
        scratch_shapes=list(scratch),
        cost_estimate=pl.CostEstimate(flops=max(flops, 1), bytes_accessed=1 << 20, transcendentals=0),
        compiler_params=pltpu.CompilerParams(vmem_limit_bytes=grant << 20),
    )(*[array for array, _ in args])


def dense_rope(block):
    return jnp.concatenate([block[0:64], block[64:128]], axis=1)


def wide_rope(block):
    return jnp.concatenate([block[:, 0:64], block[:, 64:128]], axis=0)


def pack(pos_hbm, x, q_hbm, g_hbm, lat_hbm, own, to1, to2, to3, lat, q, g, heads, pos, sems):
    copies = [
        pltpu.make_async_copy(q_hbm, q, sems.at[0]),
        pltpu.make_async_copy(g_hbm, g, sems.at[1]),
        pltpu.make_async_copy(lat_hbm, lat.at[0:576], sems.at[2]),
        pltpu.make_async_copy(pos_hbm, pos, sems.at[3]),
    ]
    for copy in copies:
        copy.start()
    copies.pop().wait()
    tag = jnp.full((16, 128), (pos[0] >> 7).astype(F32), F32).astype(BF)
    lat[576:592] = tag
    for copy in copies:
        copy.wait()
    for h in range(4):
        heads[h, 0:128] = q[:, 192 * h : 192 * h + 128]
        heads[h, 128:256] = g[:, 128 * h : 128 * h + 128]
        heads[h, 256:320] = dense_rope(q[:, 192 * h + 128 : 192 * h + 192])
        heads[h, 320:336] = tag
    for r, out in enumerate((own, to1, to2, to3)):
        out[...] = heads[(x[0] + r) & 3]


def masked_scores(raw, qtags, ktags, late):
    rows = []
    for kb in range(NK // 128):
        cols = []
        for qb in range(TQ // 128):
            part = raw[128 * kb : 128 * kb + 128, 128 * qb : 128 * qb + 128]
            seen = late <= (qtags[qb] - ktags[kb]) * 128.0
            cols.append(jnp.where(seen, part * SCALE2, NEG))
        rows.append(jnp.concatenate(cols, axis=1))
    return jnp.concatenate(rows, axis=0)


def lateness():
    shape = (128, 128)
    return (lax.broadcasted_iota(jnp.int32, shape, 0) - lax.broadcasted_iota(jnp.int32, shape, 1)).astype(F32)


NT = (((1,), (1,)), ((), ()))
NN = (((1,), (0,)), ((), ()))


def mm(a, b, dims):
    return lax.dot_general(a, b, dims, preferred_element_type=F32)


def take_queries(blocks, qp, do, qtag):
    zeros = jnp.zeros((128, 64), BF)
    for n, block in enumerate(blocks):
        at = 128 * n
        qp[at : at + 128, 0:128] = block[0:128]
        qp[at : at + 128, 128:256] = jnp.concatenate([wide_rope(block[256:320]), zeros], axis=1)
        do[at : at + 128] = block[128:256]
        qtag[0:8, at : at + 128] = block[320:336].astype(F32)[0:8]


def statistics(rows, qp, do, qtag, kp, v, ktag, stats, first):
    late = lateness()
    ktags = [ktag[8 * n : 8 * n + 1] for n in range(8)]
    stats[...] = jnp.zeros_like(stats)

    def turn(i, carry):
        at = pl.multiple_of(i * TQ, TQ)
        to = pl.multiple_of(first + i * TQ, TQ)
        raw = mm(kp[...], qp[pl.ds(at, TQ)], NT)
        qt = qtag[0:1, pl.ds(at, TQ)]
        s = masked_scores(raw, [qt[:, 0:128], qt[:, 128:256]], ktags, late)
        top = jnp.max(s, axis=0, keepdims=True)
        p = jnp.exp2(s - top)
        dp = mm(v[...], do[pl.ds(at, TQ)], NT)
        stats[0:1, pl.ds(to, TQ)] = top
        stats[1:2, pl.ds(to, TQ)] = jnp.sum(p, axis=0, keepdims=True)
        stats[2:3, pl.ds(to, TQ)] = jnp.sum(p * dp, axis=0, keepdims=True)
        return carry

    lax.fori_loop(0, rows // TQ, turn, 0)


def copied(pairs, sems, first=0):
    copies = [pltpu.make_async_copy(src, dst, sems.at[first + n]) for n, (src, dst) in enumerate(pairs)]
    for copy in copies:
        copy.start()
    return copies


def forward_own(
    core, x, q0, q1, pair, lp, lpe, lh, lhe, ku, vu,
    qp_hbm, do_hbm, qtag_hbm, compt_hbm, kpt_hbm, kp_hbm, v_hbm, ktag_hbm, kp, v, ktag, stats,
    qp, do, qtag, compt, kpt, sems, late_sems,
):
    take_queries([ref[i] for ref in (q0, q1) for i in range(2)], qp, do, qtag)
    first = core[0] == 0
    head = pl.ds(pl.multiple_of((x[0] & 3) * 128, 128), 128)
    for n in range(8):
        if n < 2:
            block = pair[n]
        elif n in (4, 5):
            mine, other = (lh, lhe) if n == 4 else (lhe, lh)
            block = jnp.where(first, mine[...], other[...])
        else:
            mine, other = (lpe, lp) if n < 4 else (lp, lpe)
            block = jnp.where(first, mine[n % 2], other[n % 2])
        at = 128 * n
        compt[:, at : at + 128] = block[0:512]
        kpt[128:192, at : at + 128] = block[512:576]
        ktag[8 * n : 8 * n + 8] = block[576:592].astype(F32)[0:8]
    kpt[192:256] = jnp.zeros((64, NK), BF)
    kpt[0:128] = mm(ku[:, head].T, compt[...], NN).astype(BF)
    pairs = [(qp, qp_hbm), (do, do_hbm), (qtag, qtag_hbm), (compt, compt_hbm), (kpt, kpt_hbm), (ktag, ktag_hbm)]
    copies = copied(pairs, sems)
    v[...] = mm(vu[:, head].T, compt[...], NN).astype(BF).T
    kp[...] = kpt[...].T
    copies += copied([(kp, kp_hbm), (v, v_hbm)], late_sems)
    statistics(512, qp, do, qtag, kp, v, ktag, stats, 0)
    for copy in copies:
        copy.wait()


def forward_near(a0, a1, b0, b1, kp, v, ktag, qp_hbm, do_hbm, qtag_hbm, stats, qp, do, qtag, sems):
    take_queries([ref[i] for ref in (b0, b1, a0, a1) for i in range(2)], qp, do, qtag)
    copies = copied([(qp, qp_hbm), (do, do_hbm), (qtag, qtag_hbm)], sems)
    statistics(1024, qp, do, qtag, kp, v, ktag, stats, 0)
    for copy in copies:
        copy.wait()


def forward_far(qc, qd, kp, v, ktag, own, near, qp_hbm, do_hbm, qtag_hbm, stats, qp, do, qtag, far, sems):
    take_queries([ref[i] for ref in (qc, qd) for i in range(2)], qp, do, qtag)
    copies = copied([(qp, qp_hbm), (do, do_hbm), (qtag, qtag_hbm)], sems)
    statistics(512, qp, do, qtag, kp, v, ktag, far, 0)
    stats[0:4] = own[0:4]
    stats[4:8] = near[0:4, 0:512]
    stats[8:12] = near[0:4, 512:1024]
    stats[12:16] = far[0:4]
    for copy in copies:
        copy.wait()


START = {0: 0, 1: 512, 3: 1024, 2: 1536}


def backward(*refs):
    there, stats, zpay, xpay, up = refs[:14], refs[14:18], refs[18:22], refs[22:26], refs[26]
    (dk, dv, low), here, sems = refs[27:30], refs[30:44], refs[44]
    kp, qp0, v, do0, ktag, qtag0, kpt, qp1, do1, qtag1, qp2, do2, qtag2, compt = here
    pairs = list(zip(there, here))
    copies = copied(pairs[:6], sems)
    late = lateness()
    for r in range(4):
        rows = []
        for d in range(4):
            at = START[(r - d) % 4] // 128
            rows.append([stats[d][at + n : at + n + 1] for n in range(3)])
        top = functools.reduce(jnp.maximum, [t[0] for t in rows])
        total = sum(t[1] * jnp.exp2(t[0] - top) for t in rows)
        weighted = sum(t[2] * jnp.exp2(t[0] - top) for t in rows)
        at = START[r]
        low[0:1, at : at + 512] = top + jnp.log2(total)
        low[1:2, at : at + 512] = weighted / total
    dk[...] = jnp.zeros_like(dk)
    dv[...] = jnp.zeros_like(dv)
    for copy in copies:
        copy.wait()
    copies += copied(pairs[6:], sems, 6)
    ktags = [ktag[8 * n : 8 * n + 1] for n in range(8)]
    for r in (0, 1, 3, 2):
        if r == 1:
            for copy in copies[7:10]:
                copy.wait()
        if r == 2:
            for copy in copies[10:13]:
                copy.wait()
        qp, do, qtag = {0: (qp0, do0, qtag0), 2: (qp2, do2, qtag2)}.get(r, (qp1, do1, qtag1))
        for i in range(2):
            to = START[r] + i * TQ
            at = i * TQ + (512 if r == 3 else 0)
            q, g, qt = qp[at : at + TQ], do[at : at + TQ], qtag[0:1, at : at + TQ]
            raw = mm(kp[...], q, NT)
            s = masked_scores(raw, [qt[:, 0:128], qt[:, 128:256]], ktags, late)
            p = jnp.exp2(s - low[0:1, to : to + TQ])
            dp = mm(v[...], g, NT)
            ds = (p * (dp - low[1:2, to : to + TQ])).astype(BF)
            dk[...] += mm(ds, q, NN)
            dv[...] += mm(p.astype(BF), g, NN)
            if to == 0:
                copies[6].wait()
            dq = (mm(kpt[...], ds, NN).T * SCALE).astype(BF)
            for b in range(2):
                m = 2 * i + b
                zpay[r][128 * m : 128 * m + 128] = dq[128 * b : 128 * b + 128, 0:128]
                zpay[r][512 + 64 * m : 576 + 64 * m] = dense_rope(dq[128 * b : 128 * b + 128, 128:192])
    dk16 = (dk[...] * SCALE).astype(BF)
    dv16 = dv[...].astype(BF)
    drope = dk16[:, 128:256].T
    for n in range(8):
        r, m = n // 2, n % 2
        xpay[r][128 * m : 128 * m + 128] = dk16[128 * n : 128 * n + 128, 0:128]
        xpay[r][256 + 128 * m : 384 + 128 * m] = dv16[128 * n : 128 * n + 128]
        xpay[r][512 + 64 * m : 576 + 64 * m] = drope[0:64, 128 * n : 128 * n + 128]
    copies[13].wait()
    both = mm(compt[...], jnp.concatenate([dk16[:, 0:128], dv16], axis=1), NN).astype(BF)
    for y in range(2):
        for z in range(4):
            at = 128 * z + 64 * y
            up[4 * y + z, 0:64] = both[at : at + 64, 0:128]
            up[4 * y + z, 64:128] = both[at : at + 64, 128:256]


def sum_queries(z0, z1, z2, z3, q0, q1, q2, q3):
    def total(rows):
        return sum(a[rows].astype(F32) for a in (z0, z1, z2, z3)).astype(BF)

    for r, back in enumerate((q0, q1, q2, q3)):
        back[0:128] = total(slice(128 * r, 128 * r + 128))
        back[128:192] = total(slice(512 + 64 * r, 576 + 64 * r))


def fold(x, x0, x1, x2, x3, ku, vu, pay, lat):
    acc = jnp.zeros((512, 256), F32)
    rope = jnp.zeros((128, 128), F32)
    for r, p in enumerate((x0, x1, x2, x3)):
        h = pl.multiple_of(lax.rem(x[0] + 4 - r, 4) * 128, 128)
        acc += mm(ku[:, pl.ds(h, 128)], p[0:256], NT)
        acc += mm(vu[:, pl.ds(h, 128)], p[256:512], NT)
        rope += p[512:640].astype(F32)
    lat[0:512] = acc[:, 0:128]
    lat[512:576] = rope[0:64]
    pay[0:512] = acc[:, 128:256].astype(BF)
    pay[512:576] = rope[64:128].astype(BF)


def spread(parts, every):
    mine = sum(parts[n].astype(F32) for n in range(8)).astype(BF)
    for n in range(32):
        every[n] = mine


def unpack_query_grad(x, q0, q1, q2, q3, out, heads):
    for r, ref in enumerate((q0, q1, q2, q3)):
        heads[(x[0] + r) & 3] = ref[...]
    for h in range(4):
        out[:, 192 * h : 192 * h + 128] = heads[h, 0:128]
        out[:, 192 * h + 128 : 192 * h + 192] = wide_rope(heads[h, 128:192])


def unpack_up(a, key, value):
    for y in range(2):
        for z in range(4):
            for x in range(4):
                part = a[place(y, z, x)].astype(F32)
                at = 128 * z + 64 * y
                key[at : at + 64, 128 * x : 128 * x + 128] = part[0:64]
                value[at : at + 64, 128 * x : 128 * x + 128] = part[64:128]


def shards(queries, latents, key_up, value_up, out_grad, positions):
    here = lax.axis_index("seq").astype(jnp.int32)
    x = here & 3
    part = ((QP, 128), BF)
    own, to1, to2, to3, lat = call(
        pack,
        [part, part, part, part, ((LP, 128), BF)],
        [(positions, HB), (x[None], SM), (queries, HB), (out_grad, HB), (latents.T, HB)],
        scratch=[
            pltpu.VMEM((ROWS, 768), BF), pltpu.VMEM((ROWS, 512), BF), pltpu.VMEM((4, QP, 128), BF),
            pltpu.SMEM((ROWS,), jnp.int32), pltpu.SemaphoreType.DMA((4,)),
        ],
    )
    core = lax.axis_index("head").astype(jnp.int32) & 1
    lat_y = along(lat, dy=1)
    q_1 = along(to1, dx=1)
    q_3 = along(to3, dx=-1)
    q_2 = along(to2, dx=2)
    pair = jnp.stack([lat, lat_y])
    q0 = jnp.stack([own, q_1])
    q1 = jnp.stack([q_2, q_3])
    lp = by_core(pair, 1)
    lh = by_core(lax.dynamic_index_in_dim(pair, core, 0, keepdims=False), 2)
    qa0 = along(q0, dz=1)
    qb0 = along(q0, dz=-1)
    qa1 = along(q1, dz=1)
    qb1 = along(q1, dz=-1)
    qc = along(qa0, dz=1)
    qd = along(qb1, dz=-1)
    lpe = to_core(lp)
    lhe = to_core(lh)

    flops = 2 * NQ * NK * 512

    def rows(n):
        return [((n, 256), BF), ((n, 128), BF), ((8, n), F32)]

    def at_hbm(shapes):
        return [(*o, HB) for o in shapes]

    def at_vmem(shapes):
        return [pltpu.VMEM(*o) for o in shapes]

    wide = [((512, NK), BF), ((256, NK), BF)]
    keyed = [((NK, 256), BF), ((NK, 128), BF), ((64, 128), F32)]
    qp0, do0, qtag0, compt, kpt, kp, v, ktag, *here, own_stats = call(
        forward_own,
        at_hbm(rows(512) + wide + keyed) + keyed + [((8, 512), F32)],
        [(core[None], SM), (x[None], SM), q0, q1, pair, lp, lpe, lh, lhe, key_up, value_up],
        scratch=at_vmem(rows(512) + wide) + [pltpu.SemaphoreType.DMA((6,)), pltpu.SemaphoreType.DMA((2,))],
        flops=flops // 4, grant=20,
    )
    qp1, do1, qtag1, near_stats = call(
        forward_near,
        at_hbm(rows(1024)) + [((8, 1024), F32)],
        [qa0, qa1, qb0, qb1, *here],
        scratch=at_vmem(rows(1024)) + [pltpu.SemaphoreType.DMA((3,))],
        flops=flops // 2, grant=14,
    )
    qp2, do2, qtag2, stats = call(
        forward_far,
        at_hbm(rows(512)) + [((16, 512), F32)],
        [qc, qd, *here, own_stats, near_stats],
        scratch=at_vmem(rows(512)) + [pltpu.VMEM((8, 512), F32), pltpu.SemaphoreType.DMA((3,))],
        flops=flops // 4, grant=12,
    )
    s1 = along(stats, dz=-1)
    s3 = along(stats, dz=1)
    s2 = along(stats, dz=2)

    there = [kp, qp0, v, do0, ktag, qtag0, kpt, qp1, do1, qtag1, qp2, do2, qtag2, compt]
    pays = call(
        backward,
        [((768, 128), BF)] * 4 + [((640, 128), BF)] * 4 + [((8, 128, 128), BF)],
        [(a, HB) for a in there] + [stats, s1, s2, s3],
        scratch=[
            pltpu.VMEM((NK, 256), F32), pltpu.VMEM((NK, 128), F32), pltpu.VMEM((8, NQ), F32),
            *[pltpu.VMEM(a.shape, a.dtype) for a in there], pltpu.SemaphoreType.DMA((14,)),
        ],
        flops=3 * flops, grant=24,
    )
    zpay, xpay, up = pays[:4], pays[4:8], pays[8]
    x1 = along(xpay[1], dx=1)
    x3 = along(xpay[3], dx=3)
    x2 = along(xpay[2], dx=2)
    ups = lax.all_to_all(up, "seq", 0, 0, tiled=True, axis_index_groups=YZ_GROUPS)
    z1 = along(zpay[1], dz=1)
    z3 = along(zpay[3], dz=3)
    z2 = along(zpay[2], dz=2)
    pay, mine = call(
        fold, [((576, 128), BF), ((576, 128), F32)],
        [(x[None], SM), xpay[0], x1, x2, x3, key_up, value_up],
        flops=2 * 256 * 512 * 1024, grant=10,
    )
    got = along(pay, dy=1)
    (every,) = call(spread, [((32, 128, 128), BF)], [ups])
    whole = lax.all_to_all(every, "seq", 0, 0, tiled=True)
    b0, b1, b2, b3 = call(sum_queries, [((192, 128), BF)] * 4, [zpay[0], z1, z2, z3])
    c1 = along(b1, dx=-1)
    c3 = along(b3, dx=-3)
    c2 = along(b2, dx=-2)
    lat16 = lax.reduce_precision(mine + got.astype(F32), 8, 7).astype(BF)
    near16 = to_core(lat16)
    two = lax.reduce_precision(lat16.astype(F32) + near16.astype(F32), 8, 7).astype(BF)
    far16 = lax.ppermute(two, "head", [(0, 2), (1, 3), (2, 0), (3, 1)])
    latent_grad = (two.astype(F32) + far16.astype(F32)).T
    (query_grad,) = call(
        unpack_query_grad, [((ROWS, 768), BF)], [(x[None], SM), b0, c1, c2, c3],
        scratch=[pltpu.VMEM((4, 192, 128), BF)],
    )
    key_up_grad, value_up_grad = call(unpack_up, [((512, 512), F32), ((512, 512), F32)], [whole])
    return (query_grad, latent_grad, key_up_grad, value_up_grad)


def solution(mesh):
    in_specs = (
        P("seq", "head"),
        P("seq", None),
        P(None, "head"),
        P(None, "head"),
        P("seq", "head"),
        P("seq"),
    )
    out_specs = (P("seq", "head"), P("seq", None), P(None, "head"), P(None, "head"))
    return jax.shard_map(shards, mesh=mesh, in_specs=in_specs, out_specs=out_specs, check_vma=False)
```
